32 devices in a mesh: dp: 16 (over z, x, core), tensor: 2 (over y).
Axes of the slice: x: 2, y: 2, z: 4, core: 2. Of those that a mesh axis runs over, the one named last changes fastest.
Arguments:
- inputs: bfloat16 [16, 256, 4096], P('dp', 'tensor'), may hold values from -40 to 40
- query_states: bfloat16 [16, 256, 3072], P('dp', None, 'tensor'), may hold values from -4.5 to 4.5
- key_states: bfloat16 [16, 256, 1024], P('dp', None, 'tensor'), may hold values from -4.5 to 4.5
- saved_value_states: bfloat16 [16, 256, 1024], P('dp', None, 'tensor'), may hold values from -4.5 to 4.5
- head_cotangent: bfloat16 [16, 256, 3072], P('dp', None, 'tensor'), may hold values from -40 to 40
- query_weight: bfloat16 [4096, 3072], P('dp', 'tensor'), may hold values from -0.09375 to 0.09375
- key_matrix: bfloat16 [4096, 1024], P('dp', 'tensor'), may hold values from -0.09375 to 0.09375
- value_matrix: bfloat16 [4096, 1024], P('dp', 'tensor'), may hold values from -0.09375 to 0.09375
- query_momentum: float32 [4096, 3072], P('dp', 'tensor'), may hold values from -6 to 6
- key_prior_momentum: float32 [4096, 1024], P('dp', 'tensor'), may hold values from -6 to 6
- value_prior_momentum: float32 [4096, 1024], P('dp', 'tensor'), may hold values from -6 to 6
Outputs:
- input_gradient: bfloat16 [16, 256, 4096], P('dp', 'tensor')
- query_velocity: float32 [4096, 3072], P('dp', 'tensor')
- key_velocity: float32 [4096, 1024], P('dp', 'tensor')
- value_velocity: float32 [4096, 1024], P('dp', 'tensor')
The draws below stay inside these ranges and needn't reach their ends.
All inputs are finite; a program needn't handle non-finite values.
Results may differ from the reference program's by a relative error of at most 0.019.
Values may be sent and summed in bfloat16 or wider, within the bound.
A program may use at most 128 MiB of HBM per device.

```python
import math
import jax
import jax.numpy as jnp
from jax import lax

MODEL_FEATURES = 4096
QUERY_HEADS = 24
KEY_VALUE_HEADS = 8
HEAD_SIZE = 128
SEQUENCE_LENGTH = 256
SEQUENCE_COUNT = 16
N_TENSOR = 2


def column_scales(base_key, width, head_width):
    spread = jnp.exp(jax.random.uniform(base_key, (width,), jnp.float32, math.log(0.3), math.log(3.0)))
    position = (jnp.arange(width, dtype=jnp.int32) // head_width).astype(jnp.float32)
    last_index = max(width // head_width - 1, 1)
    rising = jnp.exp(math.log(3.0) * (position / last_index - 0.5))
    return (spread, rising)


def draw_scaled(base_key, array_shape, head_width):
    key_scale, key_noise = jax.random.split(base_key, 2)
    width = array_shape[-1]
    spread, rising = column_scales(key_scale, width, head_width)
    value_entries = jnp.clip(jax.random.normal(key_noise, array_shape, jnp.float32), -4.0, 4.0) * spread * rising
    return value_entries


def draw_inputs(key, part):
    return draw_scaled(jax.random.fold_in(key, 11), (SEQUENCE_COUNT, SEQUENCE_LENGTH, MODEL_FEATURES), 1).astype(jnp.bfloat16)


def draw_head_cotangent(key, part):
    return draw_scaled(jax.random.fold_in(key, 13), (SEQUENCE_COUNT, SEQUENCE_LENGTH, QUERY_HEADS * HEAD_SIZE), HEAD_SIZE).astype(jnp.bfloat16)


def draw_query_states(key, part):
    base_key = jax.random.fold_in(key, 17)
    array_shape = (SEQUENCE_COUNT, SEQUENCE_LENGTH, QUERY_HEADS, HEAD_SIZE)
    value_entries = jnp.clip(jax.random.normal(base_key, array_shape, jnp.float32), -4.5, 4.5)
    return value_entries.reshape(SEQUENCE_COUNT, SEQUENCE_LENGTH, QUERY_HEADS * HEAD_SIZE).astype(jnp.bfloat16)


def draw_key_states(key, part):
    base_key = jax.random.fold_in(key, 19)
    array_shape = (SEQUENCE_COUNT, SEQUENCE_LENGTH, KEY_VALUE_HEADS, HEAD_SIZE)
    value_entries = jnp.clip(jax.random.normal(base_key, array_shape, jnp.float32), -4.5, 4.5)
    return value_entries.reshape(SEQUENCE_COUNT, SEQUENCE_LENGTH, KEY_VALUE_HEADS * HEAD_SIZE).astype(jnp.bfloat16)


def block_levels(own_key, extent, cuts, low, top_value):
    gain, own = 1.0, jax.random.fold_in(own_key, 6)
    for dim, shards_of in cuts:
        draws = jnp.exp(jax.random.uniform(jax.random.fold_in(own, dim), (shards_of,), jnp.float32, low / len(cuts), top_value / len(cuts)))
        gain = gain * jnp.repeat(draws, extent[dim] // shards_of).reshape([-1 if axis == dim else 1 for axis in range(len(extent))])
    return gain


def scatter_about(rng, extent, deviation, limit, shards=(), kind=jnp.bfloat16):
    values = deviation * jax.random.normal(rng, extent, jnp.float32)
    if shards:
        values = values * block_levels(rng, extent, shards, -0.22, 0.18)
    return jnp.clip(values, -limit, limit).astype(kind)


def setup_inputs(seed: int = 0) -> dict:
    arg_keys = jax.random.split(jax.random.key(seed), 12)
    return {
        "inputs": draw_inputs(jax.random.fold_in(arg_keys[11], 71), 0),
        "query_states": draw_query_states(jax.random.fold_in(arg_keys[11], 71), 0),
        "key_states": draw_key_states(jax.random.fold_in(arg_keys[11], 71), 0),
        "saved_value_states": scatter_about(arg_keys[3], (SEQUENCE_COUNT, SEQUENCE_LENGTH, KEY_VALUE_HEADS * HEAD_SIZE), 1.0, 4.5, ((0, 16), (2, 2))),
        "head_cotangent": draw_head_cotangent(jax.random.fold_in(arg_keys[11], 71), 0),
        "query_weight": scatter_about(arg_keys[5], (MODEL_FEATURES, QUERY_HEADS * HEAD_SIZE), MODEL_FEATURES ** -0.5, 0.09375, ((0, 16), (1, 2))),
        "key_matrix": scatter_about(arg_keys[6], (MODEL_FEATURES, KEY_VALUE_HEADS * HEAD_SIZE), MODEL_FEATURES ** -0.5, 0.09375, ((0, 16), (1, 2))),
        "value_matrix": scatter_about(arg_keys[7], (MODEL_FEATURES, KEY_VALUE_HEADS * HEAD_SIZE), MODEL_FEATURES ** -0.5, 0.09375, ((0, 16), (1, 2))),
        "query_momentum": scatter_about(arg_keys[8], (MODEL_FEATURES, QUERY_HEADS * HEAD_SIZE), 1.0, 6.0, ((0, 16), (1, 2)), jnp.float32),
        "key_prior_momentum": scatter_about(arg_keys[9], (MODEL_FEATURES, KEY_VALUE_HEADS * HEAD_SIZE), 1.0, 6.0, ((0, 16), (1, 2)), jnp.float32),
        "value_prior_momentum": scatter_about(arg_keys[10], (MODEL_FEATURES, KEY_VALUE_HEADS * HEAD_SIZE), 1.0, 6.0, ((0, 16), (1, 2)), jnp.float32),
    }


def rounded(value_entries):
    return lax.optimization_barrier(value_entries.astype(jnp.bfloat16)).astype(jnp.float32)

def sequence_backward(sequence_queries, sequence_keys, sequence_values, sequence_cotangent):
    token_length = sequence_queries.shape[0]
    group_width = QUERY_HEADS // KEY_VALUE_HEADS
    scaling = 1.0 / math.sqrt(HEAD_SIZE)
    query_quad = sequence_queries.astype(jnp.float32).reshape(token_length, KEY_VALUE_HEADS, group_width, HEAD_SIZE)
    cotangent_quad = sequence_cotangent.astype(jnp.float32).reshape(token_length, KEY_VALUE_HEADS, group_width, HEAD_SIZE)
    key_triple = sequence_keys.astype(jnp.float32).reshape(token_length, KEY_VALUE_HEADS, HEAD_SIZE)
    value_triple = sequence_values.astype(jnp.float32).reshape(token_length, KEY_VALUE_HEADS, HEAD_SIZE)
    scores = jnp.einsum('ihgd,jhd->hgij', query_quad, key_triple) * scaling
    position = jnp.arange(token_length, dtype=jnp.int32)
    causal = position[:, None] >= position[None, :]
    scores = jnp.where(causal, scores, -jnp.inf)
    maximum = lax.optimization_barrier(jnp.max(scores, axis=-1, keepdims=True))
    exponent = jnp.exp(scores - maximum)
    softmax_rows = exponent / lax.optimization_barrier(jnp.sum(exponent, axis=-1, keepdims=True))
    softmax_reduced = rounded(softmax_rows)
    grad_softmax = jnp.einsum('ihgd,jhd->hgij', cotangent_quad, value_triple)
    row_delta = lax.optimization_barrier(jnp.sum(softmax_rows * grad_softmax, axis=-1, keepdims=True))
    score_gradient = rounded(softmax_rows * (grad_softmax - row_delta) * scaling)
    grad_query = jnp.einsum('hgij,jhd->ihgd', score_gradient, key_triple).astype(jnp.bfloat16).reshape(token_length, QUERY_HEADS * HEAD_SIZE)
    key_gradient = jnp.einsum('xfwo,wxfp->oxp', score_gradient, query_quad).astype(jnp.bfloat16).reshape(token_length, KEY_VALUE_HEADS * HEAD_SIZE)
    value_gradient = jnp.einsum('xfwo,wxfp->oxp', softmax_reduced, cotangent_quad).astype(jnp.bfloat16).reshape(token_length, KEY_VALUE_HEADS * HEAD_SIZE)
    return (grad_query, key_gradient, value_gradient)

def reference(inputs, query_states, key_states, saved_value_states, head_cotangent, query_weight, key_matrix, value_matrix, query_momentum, key_prior_momentum, value_prior_momentum):
    query_share = QUERY_HEADS * HEAD_SIZE // N_TENSOR
    paired_portion = KEY_VALUE_HEADS * HEAD_SIZE // N_TENSOR

    def one_sequence(running, sequence_slices):
        input_seq, sequence_queries, sequence_keys, sequence_values, sequence_cotangent = sequence_slices
        grad_query, key_gradient, value_gradient = sequence_backward(sequence_queries, sequence_keys, sequence_values, sequence_cotangent)
        summed = jnp.zeros((input_seq.shape[0], MODEL_FEATURES), jnp.float32)
        for block_index in range(N_TENSOR):
            query_span = slice(block_index * query_share, (block_index + 1) * query_share)
            pair_span = slice(block_index * paired_portion, (block_index + 1) * paired_portion)
            partial_value = jnp.dot(grad_query[:, query_span], query_weight[:, query_span].T, preferred_element_type=jnp.float32)
            partial_value = partial_value + jnp.dot(key_gradient[:, pair_span], key_matrix[:, pair_span].T, preferred_element_type=jnp.float32)
            partial_value = partial_value + jnp.dot(value_gradient[:, pair_span], value_matrix[:, pair_span].T, preferred_element_type=jnp.float32)
            summed = summed + rounded(partial_value)
        running_query, running_key, running_value = running
        input_trans = input_seq.T
        running_query = running_query + rounded(jnp.dot(input_trans, grad_query, preferred_element_type=jnp.float32))
        running_key = running_key + rounded(jnp.dot(input_trans, key_gradient, preferred_element_type=jnp.float32))
        running_value = running_value + rounded(jnp.dot(input_trans, value_gradient, preferred_element_type=jnp.float32))
        return ((running_query, running_key, running_value), summed.astype(jnp.bfloat16))
    initial_state = (jnp.zeros((MODEL_FEATURES, QUERY_HEADS * HEAD_SIZE), jnp.float32), jnp.zeros((MODEL_FEATURES, KEY_VALUE_HEADS * HEAD_SIZE), jnp.float32), jnp.zeros((MODEL_FEATURES, KEY_VALUE_HEADS * HEAD_SIZE), jnp.float32))
    sums, input_gradient = lax.scan(one_sequence, initial_state, (inputs, query_states, key_states, saved_value_states, head_cotangent))
    grad_w_query, grad_w_key, grad_w_value = sums
    squared_total = jnp.sum(grad_w_query * grad_w_query) + jnp.sum(grad_w_key * grad_w_key) + jnp.sum(grad_w_value * grad_w_value)
    root_mean_square = jnp.sqrt(squared_total / (MODEL_FEATURES * (QUERY_HEADS + 2 * KEY_VALUE_HEADS) * HEAD_SIZE))
    factor = 1.0 / jnp.maximum(root_mean_square, 1.0)
    query_velocity = 0.9 * query_momentum + factor * grad_w_query
    key_velocity = 0.9 * key_prior_momentum + factor * grad_w_key
    value_velocity = 0.9 * value_prior_momentum + factor * grad_w_value
    return (input_gradient, query_velocity, key_velocity, value_velocity)
```

```python
import functools
import math

import jax
import jax.numpy as jnp
from jax import lax
from jax.experimental import pallas as pl
from jax.experimental.pallas import tpu as pltpu
from jax.sharding import PartitionSpec as P

HEAD_SIZE = 128
MESH = pl.DeviceIdType.MESH
F32 = jnp.float32
BF16 = jnp.bfloat16
W_FIRST = 1


def dot(a, b, ca, cb):
    return lax.dot_general(a, b, (((ca,), (cb,)), ((), ())), preferred_element_type=F32)


def kernel(
    nd, total_entries,
    x_ref, q_ref, k_ref, v_ref, do_ref, wq_ref, wk_ref, wv_ref,
    dx_ref, dwq_ref, dwk_ref, dwv_ref, fac_ref,
    g_all, x_all, w_cat, acc, part, p_buf, y_buf, d_buf, ws, wr, sq,
    xs_s, xs_r, xy_s, xy_r, w_s, w_r, col_s, col_r, xn_s, xn_r, dd_s, dd_r,
    py_s, py_r, dx_s, dx_r, dw_s, dw_r, sq_s, sq_r,
):
    kv = g_all.shape[0]
    group = g_all.shape[1]
    seq = g_all.shape[2]
    wide = g_all.shape[3]
    grp = q_ref.shape[2] // k_ref.shape[2]
    gq = grp * HEAD_SIZE
    rows = wq_ref.shape[0]
    half = seq // 2
    near = group // 2
    nz = nd // 4
    d = lax.axis_index("dp")
    t = lax.axis_index("tensor")
    c = d % 2
    xx = (d // 2) % 2
    z = d // 4

    def other_half(e):
        return e + 4 * (1 - 2 * ((e // 4) % 2))

    def member(r):
        zr = nz - 1 - z if r & 4 else z
        xr = 1 - xx if r & 2 else xx
        cr = 1 - c if r & 1 else c
        return (zr * 2 + xr) * 2 + cr

    def columns(e):
        return pl.ds(pl.multiple_of(e * rows, 128), rows)

    def to(dp, tt):
        return {"dp": dp, "tensor": tt}

    def rcopy(src, dst, ss, rs, dev):
        return pltpu.make_async_remote_copy(
            src_ref=src, dst_ref=dst, send_sem=ss, recv_sem=rs, device_id=dev, device_id_type=MESH
        )

    far = other_half(d)
    me = d * 2 + t
    total_devices = nd * 2
    bar = pltpu.get_barrier_semaphore()

    def sig(i, _):
        e = (me + i) % total_devices
        pl.semaphore_signal(bar, inc=1, device_id=to(e // 2, e % 2), device_id_type=MESH)
        return 0

    lax.fori_loop(1, total_devices, sig, 0)

    for j in range(kv):
        w_cat[j, 0:rows, 0:gq] = wq_ref[:, j * gq:(j + 1) * gq]
        w_cat[j, 0:rows, gq:gq + HEAD_SIZE] = wk_ref[:, j * HEAD_SIZE:(j + 1) * HEAD_SIZE]
        w_cat[j, 0:rows, gq + HEAD_SIZE:wide] = wv_ref[:, j * HEAD_SIZE:(j + 1) * HEAD_SIZE]

    pl.semaphore_wait(bar, total_devices - 1)

    def xcopy(r, f):
        e = member(r)
        src = e if f == 0 else other_half(e)
        return rcopy(
            x_ref.at[0, :, columns(src)], x_all.at[r, t, :, f * rows:(f + 1) * rows],
            xs_s.at[r, f], xs_r.at[r, f], to(e, t),
        )

    def xfwd(r):
        return rcopy(x_all.at[r, t], x_all.at[r, t], xy_s.at[r], xy_r.at[r], to(d, 1 - t))

    def xfwd_wait(r):
        rcopy(x_all.at[r, 1 - t], x_all.at[r, 1 - t], xy_s.at[r], xy_r.at[r], to(d, 1 - t)).wait_recv()

    def wcopy(j):
        return rcopy(
            w_cat.at[j, 0:rows], w_cat.at[j, rows:2 * rows], w_s.at[j], w_r.at[j], to(far, t)
        )

    def colcopy(j):
        return rcopy(g_all.at[j, 0], g_all.at[j, 4], col_s.at[j], col_r.at[j], to(member(4), t))

    def xncopy(i, j):
        return rcopy(
            g_all.at[j, 4 * i], g_all.at[j, 4 * i + 2], xn_s.at[i, j], xn_r.at[i, j], to(member(2), t)
        )

    def ddcopy(i, j):
        return rcopy(
            g_all.at[j, 2 * i], g_all.at[j, 2 * i + 1], dd_s.at[i, j], dd_r.at[i, j], to(member(1), t)
        )

    for r in (4, 5, 6, 7, 2, 3, 1):
        for f in range(2):
            xcopy(r, f).start()
    for f, e in ((0, d), (1, far)):
        x_all[0, t, :, f * rows:(f + 1) * rows] = x_ref[0, :, columns(e)]
    xfwd(0).start()
    for j in range(W_FIRST):
        wcopy(j).start()

    scaling = 1.0 / math.sqrt(HEAD_SIZE)

    def attention(j, _):
        kk = k_ref[0, :, pl.ds(pl.multiple_of(j * HEAD_SIZE, 128), HEAD_SIZE)]
        vv = v_ref[0, :, pl.ds(pl.multiple_of(j * HEAD_SIZE, 128), HEAD_SIZE)]
        dk = jnp.zeros((seq, HEAD_SIZE), F32)
        dv = jnp.zeros((seq, HEAD_SIZE), F32)
        mask = lax.broadcasted_iota(jnp.int32, (seq, seq), 0) >= lax.broadcasted_iota(
            jnp.int32, (seq, seq), 1
        )
        for g in range(grp):
            cols = pl.ds(pl.multiple_of(j * gq + g * HEAD_SIZE, 128), HEAD_SIZE)
            qq = q_ref[0, :, cols]
            oo = do_ref[0, :, cols]
            s = jnp.where(mask, dot(qq, kk, 1, 1) * scaling, -jnp.inf)
            e = jnp.exp(s - jnp.max(s, axis=-1, keepdims=True))
            soft = e / jnp.sum(e, axis=-1, keepdims=True)
            gs = dot(oo, vv, 1, 1)
            delta = jnp.sum(soft * gs, axis=-1, keepdims=True)
            ds = (soft * (gs - delta) * scaling).astype(BF16)
            g_all[j, 0, :, g * HEAD_SIZE:(g + 1) * HEAD_SIZE] = dot(ds, kk, 1, 0).astype(BF16)
            dk = dk + dot(ds, qq, 0, 0)
            dv = dv + dot(soft.astype(BF16), oo, 0, 0)
        g_all[j, 0, :, gq:gq + HEAD_SIZE] = dk.astype(BF16)
        g_all[j, 0, :, gq + HEAD_SIZE:wide] = dv.astype(BF16)
        colcopy(j).start()
        xncopy(0, j).start()
        ddcopy(0, j).start()
        return 0

    lax.fori_loop(0, kv, attention, 0)
    for j in range(W_FIRST, kv):
        wcopy(j).start()

    def xready(r):
        for f in range(2):
            xcopy(r, f).wait_recv()
        xfwd(r).start()

    for r in range(1, group):
        xready(r)

    def neighbours(j, _):
        xncopy(0, j).wait_recv()
        ddcopy(1, j).start()
        ddcopy(0, j).wait_recv()
        return 0

    lax.fori_loop(0, kv, neighbours, 0)
    for r in range(group):
        xfwd_wait(r)

    def near_weights(j, _):
        ddcopy(1, j).wait_recv()
        acc[j] = dot(x_all[0:near].reshape(near * seq, 2 * rows), g_all[j, 0:near].reshape(near * seq, wide), 0, 0)
        return 0

    lax.fori_loop(0, kv, near_weights, 0)

    def partial(j, lo):
        gs = g_all[j, lo:lo + near].reshape(near * seq, wide)
        return dot(gs, w_cat[j], 1, 1)

    def near_inputs(j, _):
        wcopy(j).wait_recv()

        @pl.when(j == 0)
        def _():
            part[...] = partial(j, 0)

        @pl.when(j > 0)
        def _():
            part[...] += partial(j, 0)

        return 0

    lax.fori_loop(0, kv, near_inputs, 0)

    def pcopy(r):
        return rcopy(p_buf.at[r, 1 - t], y_buf.at[r], py_s.at[r], py_r.at[r], to(d, 1 - t))

    def exchange(lo):
        for r in range(near):
            p_buf[lo + r] = part[r * seq:(r + 1) * seq].astype(BF16).reshape(2, half, 2 * rows)
            pcopy(lo + r).start()

    exchange(0)

    def dxcopy(r, f):
        e = d if f == 0 else far
        return rcopy(
            d_buf.at[r, :, f * rows:(f + 1) * rows], dx_ref.at[0, :, columns(e)],
            dx_s.at[r, f], dx_r.at[r, f], to(member(r), t),
        )

    def dxwait(r, f):
        e = member(r)
        e = e if f == 0 else other_half(e)
        rcopy(
            d_buf.at[r, :, f * rows:(f + 1) * rows], dx_ref.at[0, :, columns(e)],
            dx_s.at[r, f], dx_r.at[r, f], to(member(r), t),
        ).wait_recv()

    def finish(r):
        pcopy(r).wait_recv()
        total = (p_buf[r, t].astype(F32) + y_buf[r].astype(F32)).astype(BF16)
        if r == 0:
            for f, e in ((0, d), (1, far)):
                dx_ref[0, :, columns(e)] = total[:, f * rows:(f + 1) * rows]
        else:
            d_buf[r] = total
            for f in range(2):
                dxcopy(r, f).start()

    def dwcopy(j):
        return rcopy(ws.at[j], wr.at[j], dw_s.at[j], dw_r.at[j], to(far, t))

    def distant(j, _):
        colcopy(j).wait_recv()
        xncopy(1, j).start()
        ddcopy(2, j).start()

        @pl.when(j == 0)
        def _():
            for r in range(near):
                finish(r)

        xncopy(1, j).wait_recv()
        ddcopy(3, j).start()
        ddcopy(2, j).wait_recv()
        ddcopy(3, j).wait_recv()
        acc[j] += dot(
            x_all[near:group].reshape(near * seq, 2 * rows),
            g_all[j, near:group].reshape(near * seq, wide), 0, 0,
        )
        ws[j] = acc[j, rows:2 * rows].astype(BF16)
        dwcopy(j).start()

        @pl.when(j == 0)
        def _():
            part[...] = partial(j, near)

        @pl.when(j > 0)
        def _():
            part[...] += partial(j, near)

        return 0

    lax.fori_loop(0, kv, distant, 0)
    exchange(near)
    for r in range(near, group):
        finish(r)

    squares = jnp.zeros((1, 1), F32)
    for j in range(kv):
        dwcopy(j).wait_recv()
        a = acc[j, 0:rows] + wr[j].astype(F32)
        acc[j, 0:rows] = a
        squares = squares + jnp.sum(a * a, keepdims=True)
    sq[me] = jnp.broadcast_to(squares, (8, 128))

    def sqcopy(e, slot):
        return rcopy(sq.at[slot], sq.at[slot], sq_s.at[e], sq_r.at[slot], to(e // 2, e % 2))

    def sqsend(i, _):
        sqcopy((me + i) % total_devices, me).start()
        return 0

    lax.fori_loop(1, total_devices, sqsend, 0)
    for j in range(kv):
        dwq_ref[:, j * gq:(j + 1) * gq] = acc[j, 0:rows, 0:gq]
        dwk_ref[:, j * HEAD_SIZE:(j + 1) * HEAD_SIZE] = acc[j, 0:rows, gq:gq + HEAD_SIZE]
        dwv_ref[:, j * HEAD_SIZE:(j + 1) * HEAD_SIZE] = acc[j, 0:rows, gq + HEAD_SIZE:wide]

    for r in range(1, group):
        for f in range(2):
            xcopy(r, f).wait_send()
            dxcopy(r, f).wait_send()
            dxwait(r, f)
    for r in range(group):
        xfwd(r).wait_send()
        pcopy(r).wait_send()

    def drain_g(j, _):
        wcopy(j).wait_send()
        dwcopy(j).wait_send()
        colcopy(j).wait_send()
        for i in range(2):
            xncopy(i, j).wait_send()
        for i in range(4):
            ddcopy(i, j).wait_send()
        return 0

    lax.fori_loop(0, kv, drain_g, 0)

    def drain(i, _):
        e = (me + i) % total_devices
        sqcopy(e, me).wait_send()
        sqcopy(e, e).wait_recv()
        return 0

    lax.fori_loop(1, total_devices, drain, 0)
    total = jnp.sum(sq[...], axis=0)
    fac_ref[...] = 1.0 / jnp.maximum(jnp.sqrt(total / total_entries), 1.0)


def fused(nd, nt, inputs, q, k, v, do, wq, wk, wv):
    seq = q.shape[1]
    kv = k.shape[2] // HEAD_SIZE
    wide = (q.shape[2] + 2 * k.shape[2]) // kv
    rows = wq.shape[0]
    half = seq // nt
    group = nd // 2
    total_entries = float(rows * nd * kv * wide * nt)
    vm = pl.BlockSpec(memory_space=pltpu.VMEM)
    dma = pltpu.SemaphoreType.DMA
    return pl.pallas_call(
        functools.partial(kernel, nd, total_entries),
        out_shape=(
            jax.ShapeDtypeStruct(inputs.shape, BF16),
            jax.ShapeDtypeStruct(wq.shape, F32),
            jax.ShapeDtypeStruct(wk.shape, F32),
            jax.ShapeDtypeStruct(wv.shape, F32),
            jax.ShapeDtypeStruct((8, 128), F32),
        ),
        in_specs=[vm] * 8,
        out_specs=(vm,) * 5,
        scratch_shapes=[
            pltpu.VMEM((kv, group, seq, wide), BF16),
            pltpu.VMEM((group, nt, half, 2 * rows), BF16),
            pltpu.VMEM((kv, 2 * rows, wide), BF16),
            pltpu.VMEM((kv, 2 * rows, wide), F32),
            pltpu.VMEM((group // 2 * seq, 2 * rows), F32),
            pltpu.VMEM((group, nt, half, 2 * rows), BF16),
            pltpu.VMEM((group, half, 2 * rows), BF16),
            pltpu.VMEM((group, half, 2 * rows), BF16),
            pltpu.VMEM((kv, rows, wide), BF16),
            pltpu.VMEM((kv, rows, wide), BF16),
            pltpu.VMEM((nd * nt, 8, 128), F32),
            dma((group, 2)), dma((group, 2)), dma((group,)), dma((group,)),
            dma((kv,)), dma((kv,)), dma((kv,)), dma((kv,)),
            dma((2, kv)), dma((2, kv)), dma((4, kv)), dma((4, kv)),
            dma((group,)), dma((group,)), dma((group, 2)), dma((group, 2)),
            dma((kv,)), dma((kv,)), dma((nd * nt,)), dma((nd * nt,)),
        ],
        compiler_params=pltpu.CompilerParams(
            collective_id=0, has_side_effects=True, vmem_limit_bytes=60 * 1024 * 1024
        ),
    )(inputs, q, k, v, do, wq, wk, wv)


def heads_backward(query_row_set, key_rows, value_rows, cotangent_rows):
    token_length = query_row_set.shape[0]
    kv_heads = key_rows.shape[1] // HEAD_SIZE
    group_width = query_row_set.shape[1] // HEAD_SIZE // kv_heads
    scaling = 1.0 / math.sqrt(HEAD_SIZE)
    query_quad = query_row_set.reshape(token_length, kv_heads, group_width, HEAD_SIZE)
    cotangent_quad = cotangent_rows.reshape(token_length, kv_heads, group_width, HEAD_SIZE)
    key_triple = key_rows.reshape(token_length, kv_heads, HEAD_SIZE)
    value_triple = value_rows.reshape(token_length, kv_heads, HEAD_SIZE)
    block_rows = min(token_length, 512)
    key_sums = jnp.zeros((token_length, kv_heads, HEAD_SIZE), F32)
    value_sums = jnp.zeros((token_length, kv_heads, HEAD_SIZE), F32)
    query_blocks = []
    for row_start in range(0, token_length, block_rows):
        row_end = row_start + block_rows
        query_block = query_quad[row_start:row_end]
        cotangent_block = cotangent_quad[row_start:row_end]
        key_block = key_triple[:row_end]
        value_block = value_triple[:row_end]
        scores = (
            jnp.einsum("ihgd,jhd->hgij", query_block, key_block, preferred_element_type=F32)
            * scaling
        )
        query_index = row_start + lax.broadcasted_iota(jnp.int32, (block_rows, row_end), 0)
        key_index = lax.broadcasted_iota(jnp.int32, (block_rows, row_end), 1)
        scores = jnp.where(query_index >= key_index, scores, -jnp.inf)
        maximum = jnp.max(scores, axis=-1, keepdims=True)
        exponent = jnp.exp(scores - maximum)
        softmax_rows = exponent / jnp.sum(exponent, axis=-1, keepdims=True)
        softmax_reduced = softmax_rows.astype(BF16)
        grad_softmax = jnp.einsum(
            "ihgd,jhd->hgij", cotangent_block, value_block, preferred_element_type=F32
        )
        row_delta = jnp.sum(softmax_rows * grad_softmax, axis=-1, keepdims=True)
        score_gradient = (softmax_rows * (grad_softmax - row_delta) * scaling).astype(BF16)
        query_blocks.append(
            jnp.einsum(
                "hgij,jhd->ihgd", score_gradient, key_block, preferred_element_type=F32
            ).astype(BF16)
        )
        key_sums = key_sums.at[:row_end].add(
            jnp.einsum(
                "xfwo,wxfp->oxp", score_gradient, query_block, preferred_element_type=F32
            )
        )
        value_sums = value_sums.at[:row_end].add(
            jnp.einsum(
                "xfwo,wxfp->oxp",
                softmax_reduced,
                cotangent_block,
                preferred_element_type=F32,
            )
        )
    grad_query = jnp.concatenate(query_blocks, axis=0).reshape(token_length, -1)
    key_gradient = key_sums.astype(BF16).reshape(token_length, -1)
    value_gradient = value_sums.astype(BF16).reshape(token_length, -1)
    return (grad_query, key_gradient, value_gradient)


def small(nd, nt, inputs, query_states, key_states, query_weight):
    seq = query_states.shape[1]
    cols = query_states.shape[2] + 2 * key_states.shape[2]
    held = nd * seq * cols * 2 + 10 * nd * seq * query_weight.shape[0]
    return nt == 2 and nd == 16 and held < 36 * 1024 * 1024


def local(nd, nt, *args):
    inputs, q, k, v, do, wq, wk, wv, mq, mk, mv = args
    if small(nd, nt, inputs, q, k, wq):
        grad_inputs, gq, gk, gv, fac = fused(nd, nt, inputs, q, k, v, do, wq, wk, wv)
        factor = fac[0, 0]
    else:
        query_cols = wq.shape[1]
        pair_cols = wk.shape[1]
        rows = wq.shape[0]
        weights = jnp.concatenate((wq, wk, wv), axis=1)
        grads = jnp.concatenate(heads_backward(q[0], k[0], v[0], do[0]), axis=1)
        all_grads = lax.all_gather(grads, "dp", axis=0, tiled=True)
        pieces = lax.all_to_all(inputs[0], "dp", 1, 0, tiled=True)
        pieces = pieces.reshape(nd, -1, rows)
        all_inputs = lax.all_gather(pieces, "tensor", axis=1, tiled=True).reshape(-1, rows)
        summed = dot(all_inputs, all_grads, 0, 0)
        parts = dot(all_grads, weights, 1, 1).astype(BF16).reshape(nd, -1, rows)
        mine = lax.psum_scatter(parts, "tensor", scatter_dimension=1, tiled=True)
        grad_inputs = lax.all_to_all(mine.reshape(-1, rows), "dp", 0, 1, tiled=True)[None]
        total = lax.psum(jnp.sum(summed * summed), ("dp", "tensor"))
        factor = 1.0 / jnp.maximum(jnp.sqrt(total / (summed.size * nd * nt)), 1.0)
        gq = summed[:, :query_cols]
        gk = summed[:, query_cols:query_cols + pair_cols]
        gv = summed[:, query_cols + pair_cols:]
    return (
        grad_inputs,
        0.9 * mq + factor * gq,
        0.9 * mk + factor * gk,
        0.9 * mv + factor * gv,
    )


def solution(mesh):
    nd, nt = mesh.shape["dp"], mesh.shape["tensor"]
    saved = P("dp", None, "tensor")
    tokens = P("dp", "tensor", None)
    weight = P("dp", "tensor")
    return jax.shard_map(
        functools.partial(local, nd, nt),
        mesh=mesh,
        in_specs=(tokens,) + (saved,) * 4 + (weight,) * 6,
        out_specs=(tokens,) + (weight,) * 3,
        check_vma=False,
    )
```

```python
import functools
import math

import jax
import jax.numpy as jnp
from jax import lax
from jax.experimental import pallas as pl
from jax.experimental.pallas import tpu as pltpu
from jax.sharding import PartitionSpec as P

HEAD_SIZE = 128
MESH = pl.DeviceIdType.MESH
F32 = jnp.float32
BF16 = jnp.bfloat16
SPLIT = 2


def dot(a, b, ca, cb):
    return lax.dot_general(a, b, (((ca,), (cb,)), ((), ())), preferred_element_type=F32)


def kernel(
    nd, total_entries,
    x_ref, q_ref, k_ref, v_ref, do_ref, wq_ref, wk_ref, wv_ref,
    dx_ref, dwq_ref, dwk_ref, dwv_ref, fac_ref,
    g_all, x_all, w_cat, acc, part, fpart, p_buf, y_buf, d_buf, ws, wr, sq,
    xs_s, xs_r, xy_s, xy_r, w_s, w_r, col_s, col_r, re_s, re_r, fd_s, fd_r, xn_s, xn_r, dd_s, dd_r,
    py_s, py_r, dx_s, dx_r, dw_s, dw_r, sq_s, sq_r,
):
    kv = g_all.shape[0]
    group = g_all.shape[1]
    half = g_all.shape[3]
    seq = 2 * half
    wide = g_all.shape[4]
    grp = q_ref.shape[2] // k_ref.shape[2]
    gq = grp * HEAD_SIZE
    rows = wq_ref.shape[0]
    sub = half // SPLIT
    near = group // 2
    nz = nd // 4
    d = lax.axis_index("dp")
    t = lax.axis_index("tensor")
    c = d % 2
    xx = (d // 2) % 2
    z = d // 4

    def other_half(e):
        return e + 4 * (1 - 2 * ((e // 4) % 2))

    def member(r):
        zr = nz - 1 - z if r & 4 else z
        xr = 1 - xx if r & 2 else xx
        cr = 1 - c if r & 1 else c
        return (zr * 2 + xr) * 2 + cr

    def columns(e):
        return pl.ds(pl.multiple_of(e * rows, 128), rows)

    def to(dp, tt):
        return {"dp": dp, "tensor": tt}

    def rcopy(src, dst, ss, rs, dev):
        return pltpu.make_async_remote_copy(
            src_ref=src, dst_ref=dst, send_sem=ss, recv_sem=rs, device_id=dev, device_id_type=MESH
        )

    far = other_half(d)
    me = d * 2 + t
    total_devices = nd * 2
    bar = pltpu.get_barrier_semaphore()

    def sig(i, _):
        e = (me + i) % total_devices
        pl.semaphore_signal(bar, inc=1, device_id=to(e // 2, e % 2), device_id_type=MESH)
        return 0

    lax.fori_loop(1, total_devices, sig, 0)

    for j in range(kv):
        w_cat[j, 0:rows, 0:gq] = wq_ref[:, j * gq:(j + 1) * gq]
        w_cat[j, 0:rows, gq:gq + HEAD_SIZE] = wk_ref[:, j * HEAD_SIZE:(j + 1) * HEAD_SIZE]
        w_cat[j, 0:rows, gq + HEAD_SIZE:wide] = wv_ref[:, j * HEAD_SIZE:(j + 1) * HEAD_SIZE]

    pl.semaphore_wait(bar, total_devices - 1)

    def xcopy(r, f):
        e = member(r)
        src = e if f == 0 else other_half(e)
        return rcopy(
            x_ref.at[0, :, columns(src)], x_all.at[r, t, :, f * rows:(f + 1) * rows],
            xs_s.at[r, f], xs_r.at[r, f], to(e, t),
        )

    def xfwd(r):
        return rcopy(x_all.at[r, t], x_all.at[r, t], xy_s.at[r], xy_r.at[r], to(d, 1 - t))

    def xfwd_wait(r):
        rcopy(x_all.at[r, 1 - t], x_all.at[r, 1 - t], xy_s.at[r], xy_r.at[r], to(d, 1 - t)).wait_recv()

    def wcopy(j):
        return rcopy(
            w_cat.at[j, 0:rows], w_cat.at[j, rows:2 * rows], w_s.at[j], w_r.at[j], to(far, t)
        )

    def piece(j, r, h):
        return g_all.at[j, r, :, pl.ds(pl.multiple_of(h * sub, sub), sub)]

    def colcopy(h, j):
        return rcopy(
            piece(j, 0, h), piece(j, 4, h), col_s.at[h, j], col_r.at[h, j], to(member(4), t)
        )

    def relay(h, j):
        return rcopy(
            piece(j, 4, h), piece(j, 6, h), re_s.at[h, j], re_r.at[h, j], to(member(2), t)
        )

    def fardd(i, h, j):
        return rcopy(
            piece(j, 4 + 2 * i, h), piece(j, 5 + 2 * i, h),
            fd_s.at[i, h, j], fd_r.at[i, h, j], to(member(1), t),
        )

    def xncopy(j):
        return rcopy(g_all.at[j, 0], g_all.at[j, 2], xn_s.at[j], xn_r.at[j], to(member(2), t))

    def ddcopy(i, j):
        return rcopy(
            g_all.at[j, 2 * i], g_all.at[j, 2 * i + 1], dd_s.at[i, j], dd_r.at[i, j], to(member(1), t)
        )

    for j in range(kv):
        wcopy(j).start()
    for r in (4, 5, 6, 7, 2, 3, 1):
        for f in range(2):
            xcopy(r, f).start()
    for f, e in ((0, d), (1, far)):
        x_all[0, t, :, f * rows:(f + 1) * rows] = x_ref[0, :, columns(e)]
    xfwd(0).start()

    scaling = 1.0 / math.sqrt(HEAD_SIZE)

    def attention(j, _):
        kk = k_ref[0, :, pl.ds(pl.multiple_of(j * HEAD_SIZE, 128), HEAD_SIZE)]
        vv = v_ref[0, :, pl.ds(pl.multiple_of(j * HEAD_SIZE, 128), HEAD_SIZE)]
        dk = jnp.zeros((seq, HEAD_SIZE), F32)
        dv = jnp.zeros((seq, HEAD_SIZE), F32)
        mask = lax.broadcasted_iota(jnp.int32, (seq, seq), 0) >= lax.broadcasted_iota(
            jnp.int32, (seq, seq), 1
        )
        for g in range(grp):
            cols = pl.ds(pl.multiple_of(j * gq + g * HEAD_SIZE, 128), HEAD_SIZE)
            qq = q_ref[0, :, cols]
            oo = do_ref[0, :, cols]
            s = jnp.where(mask, dot(qq, kk, 1, 1) * scaling, -jnp.inf)
            e = jnp.exp(s - jnp.max(s, axis=-1, keepdims=True))
            soft = e / jnp.sum(e, axis=-1, keepdims=True)
            gs = dot(oo, vv, 1, 1)
            delta = jnp.sum(soft * gs, axis=-1, keepdims=True)
            ds = (soft * (gs - delta) * scaling).astype(BF16)
            g_all[j, 0, :, :, g * HEAD_SIZE:(g + 1) * HEAD_SIZE] = (
                dot(ds, kk, 1, 0).astype(BF16).reshape(2, half, HEAD_SIZE)
            )
            dk = dk + dot(ds, qq, 0, 0)
            dv = dv + dot(soft.astype(BF16), oo, 0, 0)
        g_all[j, 0, :, :, gq:gq + HEAD_SIZE] = dk.astype(BF16).reshape(2, half, HEAD_SIZE)
        g_all[j, 0, :, :, gq + HEAD_SIZE:wide] = dv.astype(BF16).reshape(2, half, HEAD_SIZE)
        colcopy(0, j).start()
        xncopy(j).start()
        ddcopy(0, j).start()
        return 0

    lax.fori_loop(0, kv, attention, 0)
    for h in range(1, SPLIT):
        for j in range(kv):
            colcopy(h, j).start()

    def xready(r):
        for f in range(2):
            xcopy(r, f).wait_recv()
        xfwd(r).start()

    for r in range(1, group):
        xready(r)

    for r in range(group):
        xfwd_wait(r)

    def pcopy(r, h):
        span = pl.ds(pl.multiple_of(h * sub, sub), sub)
        return rcopy(
            p_buf.at[r, 1 - t, span], y_buf.at[r, span], py_s.at[r, h], py_r.at[r, h], to(d, 1 - t)
        )

    def dxcopy(r, f, h, e):
        span = pl.ds(pl.multiple_of(h * sub, sub), sub)
        return rcopy(
            d_buf.at[r, span, f * rows:(f + 1) * rows], dx_ref.at[0, span, columns(e)],
            dx_s.at[r, f, h], dx_r.at[r, f, h], to(member(r), t),
        )

    def finish(r, h):
        span = pl.ds(pl.multiple_of(h * sub, sub), sub)
        pcopy(r, h).wait_recv()
        total = (p_buf[r, t, span].astype(F32) + y_buf[r, span].astype(F32)).astype(BF16)
        if r == 0:
            for f, e in ((0, d), (1, far)):
                dx_ref[0, span, columns(e)] = total[:, f * rows:(f + 1) * rows]
        else:
            d_buf[r, span] = total
            for f, e in ((0, d), (1, far)):
                dxcopy(r, f, h, e).start()

    def dwcopy(j):
        return rcopy(ws.at[j], wr.at[j], dw_s.at[j], dw_r.at[j], to(far, t))

    def receive(i):
        h = i // kv
        j = i % kv
        colcopy(h, j).wait_recv()
        relay(h, j).start()
        fardd(0, h, j).start()

        @pl.when(h == 0)
        def _():
            xncopy(j).wait_recv()
            ddcopy(1, j).start()

    def close(j):
        ddcopy(0, j).wait_recv()
        ddcopy(1, j).wait_recv()
        wcopy(j).wait_recv()
        gs = g_all[j, 0:near].reshape(near * seq, wide)
        acc[j] = dot(x_all[0:near].reshape(near * seq, 2 * rows), gs, 0, 0)
        new = dot(gs, w_cat[j], 1, 1)

        @pl.when(j == 0)
        def _():
            part[...] = new

        @pl.when(j > 0)
        def _():
            part[...] += new

    def distant(i):
        h = i // kv
        j = i % kv
        span = pl.ds(pl.multiple_of(h * sub, sub), sub)
        relay(h, j).wait_recv()
        fardd(1, h, j).start()

        @pl.when(h == 0)
        def _():
            close(j)

        fardd(0, h, j).wait_recv()
        fardd(1, h, j).wait_recv()
        gs = g_all[j, near:group, :, span].reshape(near * 2 * sub, wide)
        acc[j] += dot(x_all[near:group, :, span].reshape(near * 2 * sub, 2 * rows), gs, 0, 0)

        @pl.when(h == SPLIT - 1)
        def _():
            ws[j] = acc[j, rows:2 * rows].astype(BF16)
            dwcopy(j).start()

        new = dot(gs, w_cat[j], 1, 1)

        @pl.when(j == 0)
        def _():
            fpart[...] = new

        @pl.when(j > 0)
        def _():
            fpart[...] += new

        @pl.when(j == kv - 1)
        def _():
            for r in range(near, group):
                lo = (r - near) * 2 * sub
                p_buf[r, :, span] = (
                    fpart[lo:lo + 2 * sub].astype(BF16).reshape(2, sub, 2 * rows)
                )
                pcopy(r, h).start()

        @pl.when(i == kv - 1)
        def _():
            for r in range(near):
                p_buf[r] = part[r * seq:(r + 1) * seq].astype(BF16).reshape(2, half, 2 * rows)
                for k in range(SPLIT):
                    pcopy(r, k).start()

    steps = SPLIT * kv

    def step(i, _):
        @pl.when(i < steps)
        def _():
            receive(i)

        @pl.when(i > 0)
        def _():
            distant(i - 1)

        @pl.when(i == kv + 1)
        def _():
            for r in range(near, group):
                finish(r, 0)

        @pl.when(i == kv + 2)
        def _():
            for r in range(near):
                for k in range(SPLIT):
                    finish(r, k)

        return 0

    lax.fori_loop(0, steps + 1, step, 0)
    for h in range(1, SPLIT):
        for r in range(near, group):
            finish(r, h)

    squares = jnp.zeros((1, 1), F32)
    for j in range(kv):
        dwcopy(j).wait_recv()
        a = acc[j, 0:rows] + wr[j].astype(F32)
        acc[j, 0:rows] = a
        squares = squares + jnp.sum(a * a, keepdims=True)
    sq[me] = jnp.broadcast_to(squares, (8, 128))

    def sqcopy(e, slot):
        return rcopy(sq.at[slot], sq.at[slot], sq_s.at[e], sq_r.at[slot], to(e // 2, e % 2))

    def sqsend(i, _):
        sqcopy((me + i) % total_devices, me).start()
        return 0

    lax.fori_loop(1, total_devices, sqsend, 0)
    for j in range(kv):
        dwq_ref[:, j * gq:(j + 1) * gq] = acc[j, 0:rows, 0:gq]
        dwk_ref[:, j * HEAD_SIZE:(j + 1) * HEAD_SIZE] = acc[j, 0:rows, gq:gq + HEAD_SIZE]
        dwv_ref[:, j * HEAD_SIZE:(j + 1) * HEAD_SIZE] = acc[j, 0:rows, gq + HEAD_SIZE:wide]

    for r in range(1, group):
        e = member(r)
        for f in range(2):
            xcopy(r, f).wait_send()
            for h in range(SPLIT):
                dxcopy(r, f, h, d).wait_send()
                dxcopy(r, f, h, e if f == 0 else other_half(e)).wait_recv()
    for r in range(group):
        xfwd(r).wait_send()
        for h in range(SPLIT):
            pcopy(r, h).wait_send()

    def drain_g(j, _):
        wcopy(j).wait_send()
        dwcopy(j).wait_send()
        xncopy(j).wait_send()
        for i in range(2):
            ddcopy(i, j).wait_send()
        for h in range(SPLIT):
            colcopy(h, j).wait_send()
            relay(h, j).wait_send()
            for i in range(2):
                fardd(i, h, j).wait_send()
        return 0

    lax.fori_loop(0, kv, drain_g, 0)

    def drain(i, _):
        e = (me + i) % total_devices
        sqcopy(e, me).wait_send()
        sqcopy(e, e).wait_recv()
        return 0

    lax.fori_loop(1, total_devices, drain, 0)
    total = jnp.sum(sq[...], axis=0)
    fac_ref[...] = 1.0 / jnp.maximum(jnp.sqrt(total / total_entries), 1.0)


def fused(nd, nt, inputs, q, k, v, do, wq, wk, wv):
    seq = q.shape[1]
    kv = k.shape[2] // HEAD_SIZE
    wide = (q.shape[2] + 2 * k.shape[2]) // kv
    rows = wq.shape[0]
    half = seq // nt
    group = nd // 2
    total_entries = float(rows * nd * kv * wide * nt)
    vm = pl.BlockSpec(memory_space=pltpu.VMEM)
    dma = pltpu.SemaphoreType.DMA
    return pl.pallas_call(
        functools.partial(kernel, nd, total_entries),
        out_shape=(
            jax.ShapeDtypeStruct(inputs.shape, BF16),
            jax.ShapeDtypeStruct(wq.shape, F32),
            jax.ShapeDtypeStruct(wk.shape, F32),
            jax.ShapeDtypeStruct(wv.shape, F32),
            jax.ShapeDtypeStruct((8, 128), F32),
        ),
        in_specs=[vm] * 8,
        out_specs=(vm,) * 5,
        scratch_shapes=[
            pltpu.VMEM((kv, group, nt, half, wide), BF16),
            pltpu.VMEM((group, nt, half, 2 * rows), BF16),
            pltpu.VMEM((kv, 2 * rows, wide), BF16),
            pltpu.VMEM((kv, 2 * rows, wide), F32),
            pltpu.VMEM((group // 2 * seq, 2 * rows), F32),
            pltpu.VMEM((group // 2 * seq // SPLIT, 2 * rows), F32),
            pltpu.VMEM((group, nt, half, 2 * rows), BF16),
            pltpu.VMEM((group, half, 2 * rows), BF16),
            pltpu.VMEM((group, half, 2 * rows), BF16),
            pltpu.VMEM((kv, rows, wide), BF16),
            pltpu.VMEM((kv, rows, wide), BF16),
            pltpu.VMEM((nd * nt, 8, 128), F32),
            dma((group, 2)), dma((group, 2)), dma((group,)), dma((group,)),
            dma((kv,)), dma((kv,)), dma((SPLIT, kv)), dma((SPLIT, kv)),
            dma((SPLIT, kv)), dma((SPLIT, kv)), dma((2, SPLIT, kv)), dma((2, SPLIT, kv)),
            dma((kv,)), dma((kv,)), dma((2, kv)), dma((2, kv)),
            dma((group, SPLIT)), dma((group, SPLIT)), dma((group, 2, SPLIT)), dma((group, 2, SPLIT)),
            dma((kv,)), dma((kv,)), dma((nd * nt,)), dma((nd * nt,)),
        ],
        compiler_params=pltpu.CompilerParams(
            collective_id=0, has_side_effects=True, vmem_limit_bytes=60 * 1024 * 1024
        ),
    )(inputs, q, k, v, do, wq, wk, wv)


def heads_backward(query_row_set, key_rows, value_rows, cotangent_rows):
    token_length = query_row_set.shape[0]
    kv_heads = key_rows.shape[1] // HEAD_SIZE
    group_width = query_row_set.shape[1] // HEAD_SIZE // kv_heads
    scaling = 1.0 / math.sqrt(HEAD_SIZE)
    query_quad = query_row_set.reshape(token_length, kv_heads, group_width, HEAD_SIZE)
    cotangent_quad = cotangent_rows.reshape(token_length, kv_heads, group_width, HEAD_SIZE)
    key_triple = key_rows.reshape(token_length, kv_heads, HEAD_SIZE)
    value_triple = value_rows.reshape(token_length, kv_heads, HEAD_SIZE)
    block_rows = min(token_length, 512)
    key_sums = jnp.zeros((token_length, kv_heads, HEAD_SIZE), F32)
    value_sums = jnp.zeros((token_length, kv_heads, HEAD_SIZE), F32)
    query_blocks = []
    for row_start in range(0, token_length, block_rows):
        row_end = row_start + block_rows
        query_block = query_quad[row_start:row_end]
        cotangent_block = cotangent_quad[row_start:row_end]
        key_block = key_triple[:row_end]
        value_block = value_triple[:row_end]
        scores = (
            jnp.einsum("ihgd,jhd->hgij", query_block, key_block, preferred_element_type=F32)
            * scaling
        )
        query_index = row_start + lax.broadcasted_iota(jnp.int32, (block_rows, row_end), 0)
        key_index = lax.broadcasted_iota(jnp.int32, (block_rows, row_end), 1)
        scores = jnp.where(query_index >= key_index, scores, -jnp.inf)
        maximum = jnp.max(scores, axis=-1, keepdims=True)
        exponent = jnp.exp(scores - maximum)
        softmax_rows = exponent / jnp.sum(exponent, axis=-1, keepdims=True)
        softmax_reduced = softmax_rows.astype(BF16)
        grad_softmax = jnp.einsum(
            "ihgd,jhd->hgij", cotangent_block, value_block, preferred_element_type=F32
        )
        row_delta = jnp.sum(softmax_rows * grad_softmax, axis=-1, keepdims=True)
        score_gradient = (softmax_rows * (grad_softmax - row_delta) * scaling).astype(BF16)
        query_blocks.append(
            jnp.einsum(
                "hgij,jhd->ihgd", score_gradient, key_block, preferred_element_type=F32
            ).astype(BF16)
        )
        key_sums = key_sums.at[:row_end].add(
            jnp.einsum(
                "xfwo,wxfp->oxp", score_gradient, query_block, preferred_element_type=F32
            )
        )
        value_sums = value_sums.at[:row_end].add(
            jnp.einsum(
                "xfwo,wxfp->oxp",
                softmax_reduced,
                cotangent_block,
                preferred_element_type=F32,
            )
        )
    grad_query = jnp.concatenate(query_blocks, axis=0).reshape(token_length, -1)
    key_gradient = key_sums.astype(BF16).reshape(token_length, -1)
    value_gradient = value_sums.astype(BF16).reshape(token_length, -1)
    return (grad_query, key_gradient, value_gradient)


def small(nd, nt, inputs, query_states, key_states, query_weight):
    seq = query_states.shape[1]
    cols = query_states.shape[2] + 2 * key_states.shape[2]
    held = nd * seq * cols * 2 + 10 * nd * seq * query_weight.shape[0]
    return nt == 2 and nd == 16 and held < 36 * 1024 * 1024


def local(nd, nt, *args):
    inputs, q, k, v, do, wq, wk, wv, mq, mk, mv = args
    if small(nd, nt, inputs, q, k, wq):
        grad_inputs, gq, gk, gv, fac = fused(nd, nt, inputs, q, k, v, do, wq, wk, wv)
        factor = fac[0, 0]
    else:
        query_cols = wq.shape[1]
        pair_cols = wk.shape[1]
        rows = wq.shape[0]
        weights = jnp.concatenate((wq, wk, wv), axis=1)
        grads = jnp.concatenate(heads_backward(q[0], k[0], v[0], do[0]), axis=1)
        all_grads = lax.all_gather(grads, "dp", axis=0, tiled=True)
        pieces = lax.all_to_all(inputs[0], "dp", 1, 0, tiled=True)
        pieces = pieces.reshape(nd, -1, rows)
        all_inputs = lax.all_gather(pieces, "tensor", axis=1, tiled=True).reshape(-1, rows)
        summed = dot(all_inputs, all_grads, 0, 0)
        parts = dot(all_grads, weights, 1, 1).astype(BF16).reshape(nd, -1, rows)
        mine = lax.psum_scatter(parts, "tensor", scatter_dimension=1, tiled=True)
        grad_inputs = lax.all_to_all(mine.reshape(-1, rows), "dp", 0, 1, tiled=True)[None]
        total = lax.psum(jnp.sum(summed * summed), ("dp", "tensor"))
        factor = 1.0 / jnp.maximum(jnp.sqrt(total / (summed.size * nd * nt)), 1.0)
        gq = summed[:, :query_cols]
        gk = summed[:, query_cols:query_cols + pair_cols]
        gv = summed[:, query_cols + pair_cols:]
    return (
        grad_inputs,
        0.9 * mq + factor * gq,
        0.9 * mk + factor * gk,
        0.9 * mv + factor * gv,
    )


def solution(mesh):
    nd, nt = mesh.shape["dp"], mesh.shape["tensor"]
    saved = P("dp", None, "tensor")
    tokens = P("dp", "tensor", None)
    weight = P("dp", "tensor")
    return jax.shard_map(
        functools.partial(local, nd, nt),
        mesh=mesh,
        in_specs=(tokens,) + (saved,) * 4 + (weight,) * 6,
        out_specs=(tokens,) + (weight,) * 3,
        check_vma=False,
    )
```

```python
import functools
import math

import jax
import jax.numpy as jnp
from jax import lax
from jax.experimental import pallas as pl
from jax.experimental.pallas import tpu as pltpu
from jax.sharding import PartitionSpec as P

HEAD_SIZE = 128
MESH = pl.DeviceIdType.MESH
F32 = jnp.float32
BF16 = jnp.bfloat16
SPLIT = 2


def dot(a, b, ca, cb):
    return lax.dot_general(a, b, (((ca,), (cb,)), ((), ())), preferred_element_type=F32)


def kernel(
    nd, total_entries,
    x_in, q_in, k_in, v_in, do_in, wq_ref, wk_ref, wv_ref, mq_ref, mk_ref, mv_ref,
    dx_out, vq_out, vk_out, vv_out,
    g_all, x_all, w_cat, acc, part, fpart, p_buf, y_buf, d_buf, ws, wr, sq, mq, mk, mv,
    x_ref, q_ref, k_ref, v_ref, do_ref, dx_ref,
    xs_s, xs_r, xy_s, xy_r, w_s, w_r, col_s, col_r, re_s, re_r, fd_s, fd_r, xn_s, xn_r, dd_s, dd_r,
    py_s, py_r, dx_s, dx_r, dw_s, dw_r, sq_s, sq_r, m_s, in_s, win_s, dxo_s, vo_s,
):
    kv = g_all.shape[0]
    group = g_all.shape[1]
    half = g_all.shape[3]
    seq = 2 * half
    wide = g_all.shape[4]
    grp = q_ref.shape[2] // k_ref.shape[2]
    gq = grp * HEAD_SIZE
    rows = wq_ref.shape[0]
    sub = half // SPLIT
    near = group // 2
    nz = nd // 4
    d = lax.axis_index("dp")
    t = lax.axis_index("tensor")
    c = d % 2
    xx = (d // 2) % 2
    z = d // 4

    def other_half(e):
        return e + 4 * (1 - 2 * ((e // 4) % 2))

    def member(r):
        zr = nz - 1 - z if r & 4 else z
        xr = 1 - xx if r & 2 else xx
        cr = 1 - c if r & 1 else c
        return (zr * 2 + xr) * 2 + cr

    def columns(e):
        return pl.ds(pl.multiple_of(e * rows, 128), rows)

    def to(dp, tt):
        return {"dp": dp, "tensor": tt}

    def rcopy(src, dst, ss, rs, dev):
        return pltpu.make_async_remote_copy(
            src_ref=src, dst_ref=dst, send_sem=ss, recv_sem=rs, device_id=dev, device_id_type=MESH
        )

    far = other_half(d)
    me = d * 2 + t
    total_devices = nd * 2
    bar = pltpu.get_barrier_semaphore()

    def sig(i, _):
        e = (me + i) % total_devices
        pl.semaphore_signal(bar, inc=1, device_id=to(e // 2, e % 2), device_id_type=MESH)
        return 0

    lax.fori_loop(1, total_devices, sig, 0)
    pieces = []
    for j in range(kv):
        cq = slice(j * gq, (j + 1) * gq)
        ck = slice(j * HEAD_SIZE, (j + 1) * HEAD_SIZE)
        for i, (src, cut, lo, hi) in enumerate((
            (wq_ref, cq, 0, gq), (wk_ref, ck, gq, gq + HEAD_SIZE), (wv_ref, ck, gq + HEAD_SIZE, wide)
        )):
            pieces.append(
                pltpu.make_async_copy(src.at[:, cut], w_cat.at[j, 0:rows, lo:hi], win_s.at[j, i])
            )
    loads = [
        pltpu.make_async_copy(src, dst, in_s.at[i])
        for i, (src, dst) in enumerate(
            ((x_in, x_ref), (k_in, k_ref), (q_in, q_ref), (v_in, v_ref), (do_in, do_ref))
        )
    ]
    for copy in (loads[0], *pieces, *loads[1:]):
        copy.start()
    momentum = [
        pltpu.make_async_copy(src, dst, m_s.at[i])
        for i, (src, dst) in enumerate(((mq_ref, mq), (mk_ref, mk), (mv_ref, mv)))
    ]
    for copy in momentum:
        copy.start()

    for copy in (loads[0], *pieces):
        copy.wait()
    pl.semaphore_wait(bar, total_devices - 1)

    def xcopy(r, f):
        e = member(r)
        src = e if f == 0 else other_half(e)
        return rcopy(
            x_ref.at[0, :, columns(src)], x_all.at[r, t, :, f * rows:(f + 1) * rows],
            xs_s.at[r, f], xs_r.at[r, f], to(e, t),
        )

    def xfwd(r):
        return rcopy(x_all.at[r, t], x_all.at[r, t], xy_s.at[r], xy_r.at[r], to(d, 1 - t))

    def xfwd_wait(r):
        rcopy(x_all.at[r, 1 - t], x_all.at[r, 1 - t], xy_s.at[r], xy_r.at[r], to(d, 1 - t)).wait_recv()

    def wcopy(j):
        return rcopy(
            w_cat.at[j, 0:rows], w_cat.at[j, rows:2 * rows], w_s.at[j], w_r.at[j], to(far, t)
        )

    def piece(j, r, h):
        return g_all.at[j, r, :, pl.ds(pl.multiple_of(h * sub, sub), sub)]

    def colcopy(h, j):
        return rcopy(
            piece(j, 0, h), piece(j, 4, h), col_s.at[h, j], col_r.at[h, j], to(member(4), t)
        )

    def relay(h, j):
        return rcopy(
            piece(j, 4, h), piece(j, 6, h), re_s.at[h, j], re_r.at[h, j], to(member(2), t)
        )

    def fardd(i, h, j):
        return rcopy(
            piece(j, 4 + 2 * i, h), piece(j, 5 + 2 * i, h),
            fd_s.at[i, h, j], fd_r.at[i, h, j], to(member(1), t),
        )

    def xncopy(j):
        return rcopy(g_all.at[j, 0], g_all.at[j, 2], xn_s.at[j], xn_r.at[j], to(member(2), t))

    def ddcopy(i, j):
        return rcopy(
            g_all.at[j, 2 * i], g_all.at[j, 2 * i + 1], dd_s.at[i, j], dd_r.at[i, j], to(member(1), t)
        )

    for j in range(kv):
        wcopy(j).start()
    for r in (4, 5, 6, 7, 2, 3, 1):
        for f in range(2):
            xcopy(r, f).start()
    for f, e in ((0, d), (1, far)):
        x_all[0, t, :, f * rows:(f + 1) * rows] = x_ref[0, :, columns(e)]
    xfwd(0).start()

    for copy in loads[1:]:
        copy.wait()
    scaling = 1.0 / math.sqrt(HEAD_SIZE)

    def attention(j, _):
        kk = k_ref[0, :, pl.ds(pl.multiple_of(j * HEAD_SIZE, 128), HEAD_SIZE)]
        vv = v_ref[0, :, pl.ds(pl.multiple_of(j * HEAD_SIZE, 128), HEAD_SIZE)]
        dk = jnp.zeros((seq, HEAD_SIZE), F32)
        dv = jnp.zeros((seq, HEAD_SIZE), F32)
        mask = lax.broadcasted_iota(jnp.int32, (seq, seq), 0) >= lax.broadcasted_iota(
            jnp.int32, (seq, seq), 1
        )
        for g in range(grp):
            cols = pl.ds(pl.multiple_of(j * gq + g * HEAD_SIZE, 128), HEAD_SIZE)
            qq = q_ref[0, :, cols]
            oo = do_ref[0, :, cols]
            s = jnp.where(mask, dot(qq, kk, 1, 1) * scaling, -jnp.inf)
            e = jnp.exp(s - jnp.max(s, axis=-1, keepdims=True))
            soft = e / jnp.sum(e, axis=-1, keepdims=True)
            gs = dot(oo, vv, 1, 1)
            delta = jnp.sum(soft * gs, axis=-1, keepdims=True)
            ds = (soft * (gs - delta) * scaling).astype(BF16)
            g_all[j, 0, :, :, g * HEAD_SIZE:(g + 1) * HEAD_SIZE] = (
                dot(ds, kk, 1, 0).astype(BF16).reshape(2, half, HEAD_SIZE)
            )
            dk = dk + dot(ds, qq, 0, 0)
            dv = dv + dot(soft.astype(BF16), oo, 0, 0)
        g_all[j, 0, :, :, gq:gq + HEAD_SIZE] = dk.astype(BF16).reshape(2, half, HEAD_SIZE)
        g_all[j, 0, :, :, gq + HEAD_SIZE:wide] = dv.astype(BF16).reshape(2, half, HEAD_SIZE)
        colcopy(0, j).start()
        xncopy(j).start()
        ddcopy(0, j).start()
        return 0

    lax.fori_loop(0, kv, attention, 0)
    for h in range(1, SPLIT):
        for j in range(kv):
            colcopy(h, j).start()

    def xready(r):
        for f in range(2):
            xcopy(r, f).wait_recv()
        xfwd(r).start()

    for r in range(1, group):
        xready(r)

    for r in range(group):
        xfwd_wait(r)

    def pcopy(r, h):
        span = pl.ds(pl.multiple_of(h * sub, sub), sub)
        return rcopy(
            p_buf.at[r, 1 - t, span], y_buf.at[r, span], py_s.at[r, h], py_r.at[r, h], to(d, 1 - t)
        )

    def dxcopy(r, f, h, e):
        span = pl.ds(pl.multiple_of(h * sub, sub), sub)
        return rcopy(
            d_buf.at[r, span, f * rows:(f + 1) * rows], dx_ref.at[0, span, columns(e)],
            dx_s.at[r, f, h], dx_r.at[r, f, h], to(member(r), t),
        )

    def finish(r, h):
        span = pl.ds(pl.multiple_of(h * sub, sub), sub)
        pcopy(r, h).wait_recv()
        total = (p_buf[r, t, span].astype(F32) + y_buf[r, span].astype(F32)).astype(BF16)
        if r == 0:
            for f, e in ((0, d), (1, far)):
                dx_ref[0, span, columns(e)] = total[:, f * rows:(f + 1) * rows]
        else:
            d_buf[r, span] = total
            for f, e in ((0, d), (1, far)):
                dxcopy(r, f, h, e).start()

    def dwcopy(j):
        return rcopy(ws.at[j], wr.at[j], dw_s.at[j], dw_r.at[j], to(far, t))

    def receive(i):
        h = i // kv
        j = i % kv
        colcopy(h, j).wait_recv()
        relay(h, j).start()
        fardd(0, h, j).start()

        @pl.when(h == 0)
        def _():
            xncopy(j).wait_recv()
            ddcopy(1, j).start()

    def close(j):
        ddcopy(0, j).wait_recv()
        ddcopy(1, j).wait_recv()
        wcopy(j).wait_recv()
        gs = g_all[j, 0:near].reshape(near * seq, wide)
        acc[j] = dot(x_all[0:near].reshape(near * seq, 2 * rows), gs, 0, 0)
        new = dot(gs, w_cat[j], 1, 1)

        @pl.when(j == 0)
        def _():
            part[...] = new

        @pl.when(j > 0)
        def _():
            part[...] += new

    def distant(i):
        h = i // kv
        j = i % kv
        span = pl.ds(pl.multiple_of(h * sub, sub), sub)
        relay(h, j).wait_recv()
        fardd(1, h, j).start()

        @pl.when(h == 0)
        def _():
            close(j)

        fardd(0, h, j).wait_recv()
        fardd(1, h, j).wait_recv()
        gs = g_all[j, near:group, :, span].reshape(near * 2 * sub, wide)
        acc[j] += dot(x_all[near:group, :, span].reshape(near * 2 * sub, 2 * rows), gs, 0, 0)

        @pl.when(h == SPLIT - 1)
        def _():
            ws[j] = acc[j, rows:2 * rows].astype(BF16)
            dwcopy(j).start()

        new = dot(gs, w_cat[j], 1, 1)

        @pl.when(j == 0)
        def _():
            fpart[...] = new

        @pl.when(j > 0)
        def _():
            fpart[...] += new

        @pl.when(j == kv - 1)
        def _():
            for r in range(near, group):
                lo = (r - near) * 2 * sub
                p_buf[r, :, span] = (
                    fpart[lo:lo + 2 * sub].astype(BF16).reshape(2, sub, 2 * rows)
                )
                pcopy(r, h).start()

        @pl.when(i == kv - 1)
        def _():
            for r in range(near):
                p_buf[r] = part[r * seq:(r + 1) * seq].astype(BF16).reshape(2, half, 2 * rows)
                for k in range(SPLIT):
                    pcopy(r, k).start()

    steps = SPLIT * kv

    def step(i, _):
        @pl.when(i < steps)
        def _():
            receive(i)

        @pl.when(i > 0)
        def _():
            distant(i - 1)

        @pl.when(i == steps)
        def _():
            for r in range(near, group):
                finish(r, 0)

        return 0

    lax.fori_loop(0, steps + 1, step, 0)
    for h in range(1, SPLIT):
        for r in range(near, group):
            finish(r, h)
    for r in range(near):
        for h in range(SPLIT):
            finish(r, h)

    squares = jnp.zeros((1, 1), F32)
    for j in range(kv):
        dwcopy(j).wait_recv()
        a = acc[j, 0:rows] + wr[j].astype(F32)
        acc[j, 0:rows] = a
        squares = squares + jnp.sum(a * a, keepdims=True)
    sq[me] = jnp.broadcast_to(squares, (1, 128))

    def sqcopy(e, slot):
        return rcopy(sq.at[slot], sq.at[slot], sq_s.at[e], sq_r.at[slot], to(e // 2, e % 2))

    def sqsend(i, _):
        sqcopy((me + i) % total_devices, me).start()
        return 0

    lax.fori_loop(1, total_devices, sqsend, 0)

    for r in range(1, group):
        e = member(r)
        for f in range(2):
            xcopy(r, f).wait_send()
            for h in range(SPLIT):
                dxcopy(r, f, h, d).wait_send()
                dxcopy(r, f, h, e if f == 0 else other_half(e)).wait_recv()
    dx_store = pltpu.make_async_copy(dx_ref, dx_out, dxo_s)
    dx_store.start()
    for r in range(group):
        xfwd(r).wait_send()
        for h in range(SPLIT):
            pcopy(r, h).wait_send()

    def drain_g(j, _):
        wcopy(j).wait_send()
        dwcopy(j).wait_send()
        xncopy(j).wait_send()
        for i in range(2):
            ddcopy(i, j).wait_send()
        for h in range(SPLIT):
            colcopy(h, j).wait_send()
            relay(h, j).wait_send()
            for i in range(2):
                fardd(i, h, j).wait_send()
        return 0

    lax.fori_loop(0, kv, drain_g, 0)

    def drain(i, _):
        e = (me + i) % total_devices
        sqcopy(e, me).wait_send()
        sqcopy(e, e).wait_recv()
        return 0

    lax.fori_loop(1, total_devices, drain, 0)
    total = jnp.sum(sq[...], axis=0)[0:1, 0:1]
    factor = 1.0 / jnp.maximum(jnp.sqrt(total / total_entries), 1.0)
    for copy in momentum:
        copy.wait()
    stores = []
    for j in range(kv):
        cq = slice(j * gq, (j + 1) * gq)
        ck = slice(j * HEAD_SIZE, (j + 1) * HEAD_SIZE)
        for i, (buf, dst, cut, lo, hi) in enumerate((
            (mq, vq_out, cq, 0, gq),
            (mk, vk_out, ck, gq, gq + HEAD_SIZE),
            (mv, vv_out, ck, gq + HEAD_SIZE, wide),
        )):
            buf[:, cut] = 0.9 * buf[:, cut] + factor * acc[j, 0:rows, lo:hi]
            stores.append(pltpu.make_async_copy(buf.at[:, cut], dst.at[:, cut], vo_s.at[j, i]))
            stores[-1].start()
    for copy in (dx_store, *stores):
        copy.wait()


def fused(nd, nt, inputs, q, k, v, do, wq, wk, wv, mq, mk, mv):
    seq = q.shape[1]
    kv = k.shape[2] // HEAD_SIZE
    wide = (q.shape[2] + 2 * k.shape[2]) // kv
    rows = wq.shape[0]
    half = seq // nt
    group = nd // 2
    total_entries = float(rows * nd * kv * wide * nt)
    dma = pltpu.SemaphoreType.DMA
    return pl.pallas_call(
        functools.partial(kernel, nd, total_entries),
        out_shape=(
            jax.ShapeDtypeStruct(inputs.shape, BF16),
            jax.ShapeDtypeStruct(wq.shape, F32),
            jax.ShapeDtypeStruct(wk.shape, F32),
            jax.ShapeDtypeStruct(wv.shape, F32),
        ),
        in_specs=[pl.BlockSpec(memory_space=pltpu.HBM)] * 11,
        out_specs=(pl.BlockSpec(memory_space=pltpu.HBM),) * 4,
        scratch_shapes=[
            pltpu.VMEM((kv, group, nt, half, wide), BF16),
            pltpu.VMEM((group, nt, half, 2 * rows), BF16),
            pltpu.VMEM((kv, 2 * rows, wide), BF16),
            pltpu.VMEM((kv, 2 * rows, wide), F32),
            pltpu.VMEM((group // 2 * seq, 2 * rows), F32),
            pltpu.VMEM((group // 2 * seq // SPLIT, 2 * rows), F32),
            pltpu.VMEM((group, nt, half, 2 * rows), BF16),
            pltpu.VMEM((group, half, 2 * rows), BF16),
            pltpu.VMEM((group, half, 2 * rows), BF16),
            pltpu.VMEM((kv, rows, wide), BF16),
            pltpu.VMEM((kv, rows, wide), BF16),
            pltpu.VMEM((nd * nt, 1, 128), F32),
            pltpu.VMEM(mq.shape, F32),
            pltpu.VMEM(mk.shape, F32),
            pltpu.VMEM(mv.shape, F32),
            pltpu.VMEM(inputs.shape, BF16),
            pltpu.VMEM(q.shape, BF16),
            pltpu.VMEM(k.shape, BF16),
            pltpu.VMEM(v.shape, BF16),
            pltpu.VMEM(do.shape, BF16),
            pltpu.VMEM(inputs.shape, BF16),
            dma((group, 2)), dma((group, 2)), dma((group,)), dma((group,)),
            dma((kv,)), dma((kv,)), dma((SPLIT, kv)), dma((SPLIT, kv)),
            dma((SPLIT, kv)), dma((SPLIT, kv)), dma((2, SPLIT, kv)), dma((2, SPLIT, kv)),
            dma((kv,)), dma((kv,)), dma((2, kv)), dma((2, kv)),
            dma((group, SPLIT)), dma((group, SPLIT)), dma((group, 2, SPLIT)), dma((group, 2, SPLIT)),
            dma((kv,)), dma((kv,)), dma((nd * nt,)), dma((nd * nt,)), dma((3,)), dma((5,)), dma((kv, 3)), dma, dma((kv, 3)),
        ],
        compiler_params=pltpu.CompilerParams(
            collective_id=0, has_side_effects=True, vmem_limit_bytes=60 * 1024 * 1024
        ),
    )(inputs, q, k, v, do, wq, wk, wv, mq, mk, mv)


def pieces_of(shape):
    axis = len(shape) - 2
    step = shape[axis] // 2
    return [(slice(None),) * axis + (slice(i * step, (i + 1) * step),) for i in range(2)]


def hand_kernel(*refs):
    ins, outs, bufs, (get_s, put_s) = refs[0:4], refs[4:8], refs[8:12], refs[12:14]
    gets, puts = [], []
    for i in range(4):
        for k, cut in enumerate(pieces_of(ins[i].shape)):
            gets.append(pltpu.make_async_copy(ins[i].at[cut], bufs[i].at[cut], get_s.at[i, k]))
            puts.append(pltpu.make_async_copy(bufs[i].at[cut], outs[i].at[cut], put_s.at[i, k]))
    for get in gets:
        get.start()
    for get, put in zip(gets, puts):
        get.wait()
        put.start()
    for put in puts:
        put.wait()


def handed(*arrays):
    hbm = pl.BlockSpec(memory_space=pltpu.HBM)
    return pl.pallas_call(
        hand_kernel,
        out_shape=tuple(jax.ShapeDtypeStruct(a.shape, a.dtype) for a in arrays),
        in_specs=[hbm] * 4,
        out_specs=(hbm,) * 4,
        scratch_shapes=[pltpu.VMEM(a.shape, a.dtype) for a in arrays]
        + [pltpu.SemaphoreType.DMA((4, 2))] * 2,
        compiler_params=pltpu.CompilerParams(vmem_limit_bytes=60 * 1024 * 1024),
    )(*arrays)


def heads_backward(query_row_set, key_rows, value_rows, cotangent_rows):
    token_length = query_row_set.shape[0]
    kv_heads = key_rows.shape[1] // HEAD_SIZE
    group_width = query_row_set.shape[1] // HEAD_SIZE // kv_heads
    scaling = 1.0 / math.sqrt(HEAD_SIZE)
    query_quad = query_row_set.reshape(token_length, kv_heads, group_width, HEAD_SIZE)
    cotangent_quad = cotangent_rows.reshape(token_length, kv_heads, group_width, HEAD_SIZE)
    key_triple = key_rows.reshape(token_length, kv_heads, HEAD_SIZE)
    value_triple = value_rows.reshape(token_length, kv_heads, HEAD_SIZE)
    block_rows = min(token_length, 512)
    key_sums = jnp.zeros((token_length, kv_heads, HEAD_SIZE), F32)
    value_sums = jnp.zeros((token_length, kv_heads, HEAD_SIZE), F32)
    query_blocks = []
    for row_start in range(0, token_length, block_rows):
        row_end = row_start + block_rows
        query_block = query_quad[row_start:row_end]
        cotangent_block = cotangent_quad[row_start:row_end]
        key_block = key_triple[:row_end]
        value_block = value_triple[:row_end]
        scores = (
            jnp.einsum("ihgd,jhd->hgij", query_block, key_block, preferred_element_type=F32)
            * scaling
        )
        query_index = row_start + lax.broadcasted_iota(jnp.int32, (block_rows, row_end), 0)
        key_index = lax.broadcasted_iota(jnp.int32, (block_rows, row_end), 1)
        scores = jnp.where(query_index >= key_index, scores, -jnp.inf)
        maximum = jnp.max(scores, axis=-1, keepdims=True)
        exponent = jnp.exp(scores - maximum)
        softmax_rows = exponent / jnp.sum(exponent, axis=-1, keepdims=True)
        softmax_reduced = softmax_rows.astype(BF16)
        grad_softmax = jnp.einsum(
            "ihgd,jhd->hgij", cotangent_block, value_block, preferred_element_type=F32
        )
        row_delta = jnp.sum(softmax_rows * grad_softmax, axis=-1, keepdims=True)
        score_gradient = (softmax_rows * (grad_softmax - row_delta) * scaling).astype(BF16)
        query_blocks.append(
            jnp.einsum(
                "hgij,jhd->ihgd", score_gradient, key_block, preferred_element_type=F32
            ).astype(BF16)
        )
        key_sums = key_sums.at[:row_end].add(
            jnp.einsum(
                "xfwo,wxfp->oxp", score_gradient, query_block, preferred_element_type=F32
            )
        )
        value_sums = value_sums.at[:row_end].add(
            jnp.einsum(
                "xfwo,wxfp->oxp",
                softmax_reduced,
                cotangent_block,
                preferred_element_type=F32,
            )
        )
    grad_query = jnp.concatenate(query_blocks, axis=0).reshape(token_length, -1)
    key_gradient = key_sums.astype(BF16).reshape(token_length, -1)
    value_gradient = value_sums.astype(BF16).reshape(token_length, -1)
    return (grad_query, key_gradient, value_gradient)


def small(nd, nt, inputs, query_states, key_states, query_weight):
    seq = query_states.shape[1]
    cols = query_states.shape[2] + 2 * key_states.shape[2]
    held = nd * seq * cols * 2 + 10 * nd * seq * query_weight.shape[0]
    return nt == 2 and nd == 16 and held < 36 * 1024 * 1024


def local(nd, nt, *args):
    inputs, q, k, v, do, wq, wk, wv, mq, mk, mv = args
    if small(nd, nt, inputs, q, k, wq):
        return handed(*fused(nd, nt, *args))
    else:
        query_cols = wq.shape[1]
        pair_cols = wk.shape[1]
        rows = wq.shape[0]
        weights = jnp.concatenate((wq, wk, wv), axis=1)
        grads = jnp.concatenate(heads_backward(q[0], k[0], v[0], do[0]), axis=1)
        all_grads = lax.all_gather(grads, "dp", axis=0, tiled=True)
        pieces = lax.all_to_all(inputs[0], "dp", 1, 0, tiled=True)
        pieces = pieces.reshape(nd, -1, rows)
        all_inputs = lax.all_gather(pieces, "tensor", axis=1, tiled=True).reshape(-1, rows)
        summed = dot(all_inputs, all_grads, 0, 0)
        parts = dot(all_grads, weights, 1, 1).astype(BF16).reshape(nd, -1, rows)
        mine = lax.psum_scatter(parts, "tensor", scatter_dimension=1, tiled=True)
        grad_inputs = lax.all_to_all(mine.reshape(-1, rows), "dp", 0, 1, tiled=True)[None]
        total = lax.psum(jnp.sum(summed * summed), ("dp", "tensor"))
        factor = 1.0 / jnp.maximum(jnp.sqrt(total / (summed.size * nd * nt)), 1.0)
        gq = summed[:, :query_cols]
        gk = summed[:, query_cols:query_cols + pair_cols]
        gv = summed[:, query_cols + pair_cols:]
    return (
        grad_inputs,
        0.9 * mq + factor * gq,
        0.9 * mk + factor * gk,
        0.9 * mv + factor * gv,
    )


def solution(mesh):
    nd, nt = mesh.shape["dp"], mesh.shape["tensor"]
    saved = P("dp", None, "tensor")
    tokens = P("dp", "tensor", None)
    weight = P("dp", "tensor")
    return jax.shard_map(
        functools.partial(local, nd, nt),
        mesh=mesh,
        in_specs=(tokens,) + (saved,) * 4 + (weight,) * 6,
        out_specs=(tokens,) + (weight,) * 3,
        check_vma=False,
    )
```

```python
import functools
import math

import jax
import jax.numpy as jnp
from jax import lax
from jax.experimental import pallas as pl
from jax.experimental.pallas import tpu as pltpu
from jax.sharding import PartitionSpec as P

HEAD_SIZE = 128
MESH = pl.DeviceIdType.MESH
F32 = jnp.float32
BF16 = jnp.bfloat16
SPLIT = 2
AHEAD = 4


def dot(a, b, ca, cb):
    return lax.dot_general(a, b, (((ca,), (cb,)), ((), ())), preferred_element_type=F32)


def kernel(
    nd, total_entries,
    x_in, q_in, k_in, v_in, do_in, wq_ref, wk_ref, wv_ref, mq_ref, mk_ref, mv_ref,
    dx_out, vq_out, vk_out, vv_out,
    g_all, x_all, w_cat, acc, part, fpart, p_buf, y_buf, d_buf, ws, wr, sq, mq, mk, mv,
    x_ref, q_ref, k_ref, v_ref, do_ref, dx_ref,
    xs_s, xs_r, xy_s, xy_r, w_s, w_r, col_s, col_r, re_s, re_r, fd_s, fd_r, xn_s, xn_r, dd_s, dd_r,
    py_s, py_r, dx_s, dx_r, dw_s, dw_r, sq_s, sq_r, m_s, in_s, win_s, dxo_s, vo_s,
):
    kv = g_all.shape[0]
    group = g_all.shape[1]
    half = g_all.shape[3]
    seq = 2 * half
    wide = g_all.shape[4]
    grp = q_ref.shape[2] // k_ref.shape[2]
    gq = grp * HEAD_SIZE
    rows = wq_ref.shape[0]
    sub = half // SPLIT
    near = group // 2
    nz = nd // 4
    d = lax.axis_index("dp")
    t = lax.axis_index("tensor")
    c = d % 2
    xx = (d // 2) % 2
    z = d // 4

    def other_half(e):
        return e + 4 * (1 - 2 * ((e // 4) % 2))

    def member(r):
        zr = nz - 1 - z if r & 4 else z
        xr = 1 - xx if r & 2 else xx
        cr = 1 - c if r & 1 else c
        return (zr * 2 + xr) * 2 + cr

    def columns(e):
        return pl.ds(pl.multiple_of(e * rows, 128), rows)

    def to(dp, tt):
        return {"dp": dp, "tensor": tt}

    def rcopy(src, dst, ss, rs, dev):
        return pltpu.make_async_remote_copy(
            src_ref=src, dst_ref=dst, send_sem=ss, recv_sem=rs, device_id=dev, device_id_type=MESH
        )

    far = other_half(d)
    outer = jnp.logical_or(z == 0, z == nz - 1)
    inner = jnp.logical_not(outer)
    me = d * 2 + t
    total_devices = nd * 2
    bar = pltpu.get_barrier_semaphore()

    def sig(i, _):
        e = (me + i) % total_devices
        pl.semaphore_signal(bar, inc=1, device_id=to(e // 2, e % 2), device_id_type=MESH)
        return 0

    lax.fori_loop(1, total_devices, sig, 0)
    pieces = []
    for j in range(kv):
        cq = slice(j * gq, (j + 1) * gq)
        ck = slice(j * HEAD_SIZE, (j + 1) * HEAD_SIZE)
        for i, (src, cut, lo, hi) in enumerate((
            (wq_ref, cq, 0, gq), (wk_ref, ck, gq, gq + HEAD_SIZE), (wv_ref, ck, gq + HEAD_SIZE, wide)
        )):
            pieces.append(
                pltpu.make_async_copy(src.at[:, cut], w_cat.at[j, 0:rows, lo:hi], win_s.at[j, i])
            )
    loads = [
        pltpu.make_async_copy(src, dst, in_s.at[i])
        for i, (src, dst) in enumerate(
            ((x_in, x_ref), (k_in, k_ref), (q_in, q_ref), (v_in, v_ref), (do_in, do_ref))
        )
    ]
    for copy in (loads[0], *pieces, *loads[1:]):
        copy.start()
    momentum = [
        pltpu.make_async_copy(src, dst, m_s.at[i])
        for i, (src, dst) in enumerate(((mq_ref, mq), (mk_ref, mk), (mv_ref, mv)))
    ]
    for copy in momentum:
        copy.start()

    for copy in (loads[0], *pieces):
        copy.wait()
    pl.semaphore_wait(bar, total_devices - 1)

    def xcopy(r, f):
        e = member(r)
        src = e if f == 0 else other_half(e)
        return rcopy(
            x_ref.at[0, :, columns(src)], x_all.at[r, t, :, f * rows:(f + 1) * rows],
            xs_s.at[r, f], xs_r.at[r, f], to(e, t),
        )

    def xfwd(r):
        return rcopy(x_all.at[r, t], x_all.at[r, t], xy_s.at[r], xy_r.at[r], to(d, 1 - t))

    def xfwd_wait(r):
        rcopy(x_all.at[r, 1 - t], x_all.at[r, 1 - t], xy_s.at[r], xy_r.at[r], to(d, 1 - t)).wait_recv()

    def wcopy(j):
        return rcopy(
            w_cat.at[j, 0:rows], w_cat.at[j, rows:2 * rows], w_s.at[j], w_r.at[j], to(far, t)
        )

    def piece(j, r, h):
        return g_all.at[j, r, :, pl.ds(pl.multiple_of(h * sub, sub), sub)]

    def colcopy(h, j):
        return rcopy(
            piece(j, 0, h), piece(j, 4, h), col_s.at[h, j], col_r.at[h, j], to(member(4), t)
        )

    def relay(h, j):
        return rcopy(
            piece(j, 4, h), piece(j, 6, h), re_s.at[h, j], re_r.at[h, j], to(member(2), t)
        )

    def fardd(i, h, j):
        return rcopy(
            piece(j, 4 + 2 * i, h), piece(j, 5 + 2 * i, h),
            fd_s.at[i, h, j], fd_r.at[i, h, j], to(member(1), t),
        )

    def xncopy(j):
        return rcopy(g_all.at[j, 0], g_all.at[j, 2], xn_s.at[j], xn_r.at[j], to(member(2), t))

    def ddcopy(i, j):
        return rcopy(
            g_all.at[j, 2 * i], g_all.at[j, 2 * i + 1], dd_s.at[i, j], dd_r.at[i, j], to(member(1), t)
        )

    for j in range(kv):
        wcopy(j).start()
    for r in (4, 5, 6, 7, 2, 3, 1):
        for f in range(2):
            xcopy(r, f).start()
    for f, e in ((0, d), (1, far)):
        x_all[0, t, :, f * rows:(f + 1) * rows] = x_ref[0, :, columns(e)]
    xfwd(0).start()

    for copy in loads[1:]:
        copy.wait()
    scaling = 1.0 / math.sqrt(HEAD_SIZE)

    def attention(j, _):
        kk = k_ref[0, :, pl.ds(pl.multiple_of(j * HEAD_SIZE, 128), HEAD_SIZE)]
        vv = v_ref[0, :, pl.ds(pl.multiple_of(j * HEAD_SIZE, 128), HEAD_SIZE)]
        dk = jnp.zeros((seq, HEAD_SIZE), F32)
        dv = jnp.zeros((seq, HEAD_SIZE), F32)
        mask = lax.broadcasted_iota(jnp.int32, (seq, seq), 0) >= lax.broadcasted_iota(
            jnp.int32, (seq, seq), 1
        )
        for g in range(grp):
            cols = pl.ds(pl.multiple_of(j * gq + g * HEAD_SIZE, 128), HEAD_SIZE)
            qq = q_ref[0, :, cols]
            oo = do_ref[0, :, cols]
            s = jnp.where(mask, dot(qq, kk, 1, 1) * scaling, -jnp.inf)
            e = jnp.exp(s - jnp.max(s, axis=-1, keepdims=True))
            soft = e / jnp.sum(e, axis=-1, keepdims=True)
            gs = dot(oo, vv, 1, 1)
            delta = jnp.sum(soft * gs, axis=-1, keepdims=True)
            ds = (soft * (gs - delta) * scaling).astype(BF16)
            g_all[j, 0, :, :, g * HEAD_SIZE:(g + 1) * HEAD_SIZE] = (
                dot(ds, kk, 1, 0).astype(BF16).reshape(2, half, HEAD_SIZE)
            )
            dk = dk + dot(ds, qq, 0, 0)
            dv = dv + dot(soft.astype(BF16), oo, 0, 0)
        g_all[j, 0, :, :, gq:gq + HEAD_SIZE] = dk.astype(BF16).reshape(2, half, HEAD_SIZE)
        g_all[j, 0, :, :, gq + HEAD_SIZE:wide] = dv.astype(BF16).reshape(2, half, HEAD_SIZE)
        colcopy(0, j).start()

        @pl.when(inner)
        def _():
            for h in range(1, SPLIT):
                colcopy(h, j).start()

        @pl.when(jnp.logical_or(outer, j < AHEAD))
        def _():
            xncopy(j).start()

        ddcopy(0, j).start()
        return 0

    lax.fori_loop(0, kv, attention, 0)

    @pl.when(outer)
    def _():
        for h in range(1, SPLIT):
            for j in range(kv):
                colcopy(h, j).start()

    def xready(r):
        for f in range(2):
            xcopy(r, f).wait_recv()
        xfwd(r).start()

    for r in range(1, group):
        xready(r)

    for r in range(group):
        xfwd_wait(r)

    steps = SPLIT * kv

    def pcopy(r, h):
        span = pl.ds(pl.multiple_of(h * sub, sub), sub)
        return rcopy(
            p_buf.at[r, 1 - t, span], y_buf.at[r, span], py_s.at[r, h], py_r.at[r, h], to(d, 1 - t)
        )

    def dxcopy(r, f, h, e):
        span = pl.ds(pl.multiple_of(h * sub, sub), sub)
        return rcopy(
            d_buf.at[r, span, f * rows:(f + 1) * rows], dx_ref.at[0, span, columns(e)],
            dx_s.at[r, f, h], dx_r.at[r, f, h], to(member(r), t),
        )

    def finish(r, h):
        span = pl.ds(pl.multiple_of(h * sub, sub), sub)
        pcopy(r, h).wait_recv()
        total = (p_buf[r, t, span].astype(F32) + y_buf[r, span].astype(F32)).astype(BF16)
        if r == 0:
            for f, e in ((0, d), (1, far)):
                dx_ref[0, span, columns(e)] = total[:, f * rows:(f + 1) * rows]
        else:
            d_buf[r, span] = total
            for f, e in ((0, d), (1, far)):
                dxcopy(r, f, h, e).start()

    def dwcopy(j):
        return rcopy(ws.at[j], wr.at[j], dw_s.at[j], dw_r.at[j], to(far, t))

    def place(i):
        return jnp.where(outer, i // kv, i % SPLIT), jnp.where(outer, i % kv, i // SPLIT)

    def receive(i):
        h, j = place(i)
        colcopy(h, j).wait_recv()
        relay(h, j).start()
        fardd(0, h, j).start()

        @pl.when(h == 0)
        def _():
            xncopy(j).wait_recv()
            ddcopy(1, j).start()

        @pl.when(jnp.logical_and(inner, jnp.logical_and(h == SPLIT - 1, j + AHEAD < kv)))
        def _():
            xncopy(j + AHEAD).start()

    def close(j):
        ddcopy(0, j).wait_recv()
        ddcopy(1, j).wait_recv()
        wcopy(j).wait_recv()
        gs = g_all[j, 0:near].reshape(near * seq, wide)
        acc[j] = dot(x_all[0:near].reshape(near * seq, 2 * rows), gs, 0, 0)
        new = dot(gs, w_cat[j], 1, 1)

        @pl.when(j == 0)
        def _():
            part[...] = new

        @pl.when(j > 0)
        def _():
            part[...] += new

    def distant(i):
        h, j = place(i)
        span = pl.ds(pl.multiple_of(h * sub, sub), sub)
        relay(h, j).wait_recv()
        fardd(1, h, j).start()

        @pl.when(h == 0)
        def _():
            close(j)

        fardd(0, h, j).wait_recv()
        fardd(1, h, j).wait_recv()
        gs = g_all[j, near:group, :, span].reshape(near * 2 * sub, wide)
        acc[j] += dot(x_all[near:group, :, span].reshape(near * 2 * sub, 2 * rows), gs, 0, 0)

        @pl.when(h == SPLIT - 1)
        def _():
            ws[j] = acc[j, rows:2 * rows].astype(BF16)
            dwcopy(j).start()

        new = dot(gs, w_cat[j], 1, 1)

        @pl.when(j == 0)
        def _():
            fpart[h] = new

        @pl.when(j > 0)
        def _():
            fpart[h] += new

        @pl.when(j == kv - 1)
        def _():
            for r in range(near, group):
                lo = (r - near) * 2 * sub
                p_buf[r, :, span] = (
                    fpart[h, lo:lo + 2 * sub].astype(BF16).reshape(2, sub, 2 * rows)
                )
                pcopy(r, h).start()

        @pl.when(i == jnp.where(outer, kv - 1, steps - 1))
        def _():
            for r in range(near):
                p_buf[r] = part[r * seq:(r + 1) * seq].astype(BF16).reshape(2, half, 2 * rows)
                for k in range(SPLIT):
                    pcopy(r, k).start()

    def step(i, _):
        @pl.when(i < steps)
        def _():
            receive(i)

        @pl.when(i > 0)
        def _():
            distant(i - 1)

        @pl.when(i == steps)
        def _():
            for r in range(near, group):
                finish(r, 0)

        return 0

    lax.fori_loop(0, steps + 1, step, 0)
    for h in range(1, SPLIT):
        for r in range(near, group):
            finish(r, h)
    for r in range(near):
        for h in range(SPLIT):
            finish(r, h)

    squares = jnp.zeros((1, 1), F32)
    for j in range(kv):
        dwcopy(j).wait_recv()
        a = acc[j, 0:rows] + wr[j].astype(F32)
        acc[j, 0:rows] = a
        squares = squares + jnp.sum(a * a, keepdims=True)
    sq[me] = jnp.broadcast_to(squares, (1, 128))

    def sqcopy(e, slot):
        return rcopy(sq.at[slot], sq.at[slot], sq_s.at[e], sq_r.at[slot], to(e // 2, e % 2))

    def sqsend(i, _):
        sqcopy((me + i) % total_devices, me).start()
        return 0

    lax.fori_loop(1, total_devices, sqsend, 0)

    for r in range(1, group):
        e = member(r)
        for f in range(2):
            xcopy(r, f).wait_send()
            for h in range(SPLIT):
                dxcopy(r, f, h, d).wait_send()
                dxcopy(r, f, h, e if f == 0 else other_half(e)).wait_recv()
    dx_store = pltpu.make_async_copy(dx_ref, dx_out, dxo_s)
    dx_store.start()
    for r in range(group):
        xfwd(r).wait_send()
        for h in range(SPLIT):
            pcopy(r, h).wait_send()

    def drain_g(j, _):
        wcopy(j).wait_send()
        dwcopy(j).wait_send()
        xncopy(j).wait_send()
        for i in range(2):
            ddcopy(i, j).wait_send()
        for h in range(SPLIT):
            colcopy(h, j).wait_send()
            relay(h, j).wait_send()
            for i in range(2):
                fardd(i, h, j).wait_send()
        return 0

    lax.fori_loop(0, kv, drain_g, 0)

    def drain(i, _):
        e = (me + i) % total_devices
        sqcopy(e, me).wait_send()
        sqcopy(e, e).wait_recv()
        return 0

    lax.fori_loop(1, total_devices, drain, 0)
    total = jnp.sum(sq[...], axis=0)[0:1, 0:1]
    factor = 1.0 / jnp.maximum(jnp.sqrt(total / total_entries), 1.0)
    for copy in momentum:
        copy.wait()
    stores = []
    for j in range(kv):
        cq = slice(j * gq, (j + 1) * gq)
        ck = slice(j * HEAD_SIZE, (j + 1) * HEAD_SIZE)
        for i, (buf, dst, cut, lo, hi) in enumerate((
            (mq, vq_out, cq, 0, gq),
            (mk, vk_out, ck, gq, gq + HEAD_SIZE),
            (mv, vv_out, ck, gq + HEAD_SIZE, wide),
        )):
            buf[:, cut] = 0.9 * buf[:, cut] + factor * acc[j, 0:rows, lo:hi]
            stores.append(pltpu.make_async_copy(buf.at[:, cut], dst.at[:, cut], vo_s.at[j, i]))
            stores[-1].start()
    for copy in (dx_store, *stores):
        copy.wait()


def fused(nd, nt, inputs, q, k, v, do, wq, wk, wv, mq, mk, mv):
    seq = q.shape[1]
    kv = k.shape[2] // HEAD_SIZE
    wide = (q.shape[2] + 2 * k.shape[2]) // kv
    rows = wq.shape[0]
    half = seq // nt
    group = nd // 2
    total_entries = float(rows * nd * kv * wide * nt)
    dma = pltpu.SemaphoreType.DMA
    return pl.pallas_call(
        functools.partial(kernel, nd, total_entries),
        out_shape=(
            jax.ShapeDtypeStruct(inputs.shape, BF16),
            jax.ShapeDtypeStruct(wq.shape, F32),
            jax.ShapeDtypeStruct(wk.shape, F32),
            jax.ShapeDtypeStruct(wv.shape, F32),
        ),
        in_specs=[pl.BlockSpec(memory_space=pltpu.HBM)] * 11,
        out_specs=(pl.BlockSpec(memory_space=pltpu.HBM),) * 4,
        scratch_shapes=[
            pltpu.VMEM((kv, group, nt, half, wide), BF16),
            pltpu.VMEM((group, nt, half, 2 * rows), BF16),
            pltpu.VMEM((kv, 2 * rows, wide), BF16),
            pltpu.VMEM((kv, 2 * rows, wide), F32),
            pltpu.VMEM((group // 2 * seq, 2 * rows), F32),
            pltpu.VMEM((SPLIT, group // 2 * seq // SPLIT, 2 * rows), F32),
            pltpu.VMEM((group, nt, half, 2 * rows), BF16),
            pltpu.VMEM((group, half, 2 * rows), BF16),
            pltpu.VMEM((group, half, 2 * rows), BF16),
            pltpu.VMEM((kv, rows, wide), BF16),
            pltpu.VMEM((kv, rows, wide), BF16),
            pltpu.VMEM((nd * nt, 1, 128), F32),
            pltpu.VMEM(mq.shape, F32),
            pltpu.VMEM(mk.shape, F32),
            pltpu.VMEM(mv.shape, F32),
            pltpu.VMEM(inputs.shape, BF16),
            pltpu.VMEM(q.shape, BF16),
            pltpu.VMEM(k.shape, BF16),
            pltpu.VMEM(v.shape, BF16),
            pltpu.VMEM(do.shape, BF16),
            pltpu.VMEM(inputs.shape, BF16),
            dma((group, 2)), dma((group, 2)), dma((group,)), dma((group,)),
            dma((kv,)), dma((kv,)), dma((SPLIT, kv)), dma((SPLIT, kv)),
            dma((SPLIT, kv)), dma((SPLIT, kv)), dma((2, SPLIT, kv)), dma((2, SPLIT, kv)),
            dma((kv,)), dma((kv,)), dma((2, kv)), dma((2, kv)),
            dma((group, SPLIT)), dma((group, SPLIT)), dma((group, 2, SPLIT)), dma((group, 2, SPLIT)),
            dma((kv,)), dma((kv,)), dma((nd * nt,)), dma((nd * nt,)), dma((3,)), dma((5,)), dma((kv, 3)), dma, dma((kv, 3)),
        ],
        compiler_params=pltpu.CompilerParams(
            collective_id=0, has_side_effects=True, vmem_limit_bytes=60 * 1024 * 1024
        ),
    )(inputs, q, k, v, do, wq, wk, wv, mq, mk, mv)


def pieces_of(shape):
    axis = len(shape) - 2
    step = shape[axis] // 2
    return [(slice(None),) * axis + (slice(i * step, (i + 1) * step),) for i in range(2)]


def hand_kernel(*refs):
    ins, outs, bufs, (get_s, put_s) = refs[0:4], refs[4:8], refs[8:12], refs[12:14]
    gets, puts = [], []
    for i in range(4):
        for k, cut in enumerate(pieces_of(ins[i].shape)):
            gets.append(pltpu.make_async_copy(ins[i].at[cut], bufs[i].at[cut], get_s.at[i, k]))
            puts.append(pltpu.make_async_copy(bufs[i].at[cut], outs[i].at[cut], put_s.at[i, k]))
    for get in gets:
        get.start()
    for get, put in zip(gets, puts):
        get.wait()
        put.start()
    for put in puts:
        put.wait()


def handed(*arrays):
    hbm = pl.BlockSpec(memory_space=pltpu.HBM)
    return pl.pallas_call(
        hand_kernel,
        out_shape=tuple(jax.ShapeDtypeStruct(a.shape, a.dtype) for a in arrays),
        in_specs=[hbm] * 4,
        out_specs=(hbm,) * 4,
        scratch_shapes=[pltpu.VMEM(a.shape, a.dtype) for a in arrays]
        + [pltpu.SemaphoreType.DMA((4, 2))] * 2,
        compiler_params=pltpu.CompilerParams(vmem_limit_bytes=60 * 1024 * 1024),
    )(*arrays)


def heads_backward(query_row_set, key_rows, value_rows, cotangent_rows):
    token_length = query_row_set.shape[0]
    kv_heads = key_rows.shape[1] // HEAD_SIZE
    group_width = query_row_set.shape[1] // HEAD_SIZE // kv_heads
    scaling = 1.0 / math.sqrt(HEAD_SIZE)
    query_quad = query_row_set.reshape(token_length, kv_heads, group_width, HEAD_SIZE)
    cotangent_quad = cotangent_rows.reshape(token_length, kv_heads, group_width, HEAD_SIZE)
    key_triple = key_rows.reshape(token_length, kv_heads, HEAD_SIZE)
    value_triple = value_rows.reshape(token_length, kv_heads, HEAD_SIZE)
    block_rows = min(token_length, 512)
    key_sums = jnp.zeros((token_length, kv_heads, HEAD_SIZE), F32)
    value_sums = jnp.zeros((token_length, kv_heads, HEAD_SIZE), F32)
    query_blocks = []
    for row_start in range(0, token_length, block_rows):
        row_end = row_start + block_rows
        query_block = query_quad[row_start:row_end]
        cotangent_block = cotangent_quad[row_start:row_end]
        key_block = key_triple[:row_end]
        value_block = value_triple[:row_end]
        scores = (
            jnp.einsum("ihgd,jhd->hgij", query_block, key_block, preferred_element_type=F32)
            * scaling
        )
        query_index = row_start + lax.broadcasted_iota(jnp.int32, (block_rows, row_end), 0)
        key_index = lax.broadcasted_iota(jnp.int32, (block_rows, row_end), 1)
        scores = jnp.where(query_index >= key_index, scores, -jnp.inf)
        maximum = jnp.max(scores, axis=-1, keepdims=True)
        exponent = jnp.exp(scores - maximum)
        softmax_rows = exponent / jnp.sum(exponent, axis=-1, keepdims=True)
        softmax_reduced = softmax_rows.astype(BF16)
        grad_softmax = jnp.einsum(
            "ihgd,jhd->hgij", cotangent_block, value_block, preferred_element_type=F32
        )
        row_delta = jnp.sum(softmax_rows * grad_softmax, axis=-1, keepdims=True)
        score_gradient = (softmax_rows * (grad_softmax - row_delta) * scaling).astype(BF16)
        query_blocks.append(
            jnp.einsum(
                "hgij,jhd->ihgd", score_gradient, key_block, preferred_element_type=F32
            ).astype(BF16)
        )
        key_sums = key_sums.at[:row_end].add(
            jnp.einsum(
                "xfwo,wxfp->oxp", score_gradient, query_block, preferred_element_type=F32
            )
        )
        value_sums = value_sums.at[:row_end].add(
            jnp.einsum(
                "xfwo,wxfp->oxp",
                softmax_reduced,
                cotangent_block,
                preferred_element_type=F32,
            )
        )
    grad_query = jnp.concatenate(query_blocks, axis=0).reshape(token_length, -1)
    key_gradient = key_sums.astype(BF16).reshape(token_length, -1)
    value_gradient = value_sums.astype(BF16).reshape(token_length, -1)
    return (grad_query, key_gradient, value_gradient)


def small(nd, nt, inputs, query_states, key_states, query_weight):
    seq = query_states.shape[1]
    cols = query_states.shape[2] + 2 * key_states.shape[2]
    held = nd * seq * cols * 2 + 10 * nd * seq * query_weight.shape[0]
    return nt == 2 and nd == 16 and held < 36 * 1024 * 1024


def local(nd, nt, *args):
    inputs, q, k, v, do, wq, wk, wv, mq, mk, mv = args
    if small(nd, nt, inputs, q, k, wq):
        return handed(*fused(nd, nt, *args))
    else:
        query_cols = wq.shape[1]
        pair_cols = wk.shape[1]
        rows = wq.shape[0]
        weights = jnp.concatenate((wq, wk, wv), axis=1)
        grads = jnp.concatenate(heads_backward(q[0], k[0], v[0], do[0]), axis=1)
        all_grads = lax.all_gather(grads, "dp", axis=0, tiled=True)
        pieces = lax.all_to_all(inputs[0], "dp", 1, 0, tiled=True)
        pieces = pieces.reshape(nd, -1, rows)
        all_inputs = lax.all_gather(pieces, "tensor", axis=1, tiled=True).reshape(-1, rows)
        summed = dot(all_inputs, all_grads, 0, 0)
        parts = dot(all_grads, weights, 1, 1).astype(BF16).reshape(nd, -1, rows)
        mine = lax.psum_scatter(parts, "tensor", scatter_dimension=1, tiled=True)
        grad_inputs = lax.all_to_all(mine.reshape(-1, rows), "dp", 0, 1, tiled=True)[None]
        total = lax.psum(jnp.sum(summed * summed), ("dp", "tensor"))
        factor = 1.0 / jnp.maximum(jnp.sqrt(total / (summed.size * nd * nt)), 1.0)
        gq = summed[:, :query_cols]
        gk = summed[:, query_cols:query_cols + pair_cols]
        gv = summed[:, query_cols + pair_cols:]
    return (
        grad_inputs,
        0.9 * mq + factor * gq,
        0.9 * mk + factor * gk,
        0.9 * mv + factor * gv,
    )


def solution(mesh):
    nd, nt = mesh.shape["dp"], mesh.shape["tensor"]
    saved = P("dp", None, "tensor")
    tokens = P("dp", "tensor", None)
    weight = P("dp", "tensor")
    return jax.shard_map(
        functools.partial(local, nd, nt),
        mesh=mesh,
        in_specs=(tokens,) + (saved,) * 4 + (weight,) * 6,
        out_specs=(tokens,) + (weight,) * 3,
        check_vma=False,
    )
```

```python
import functools
import math

import jax
import jax.numpy as jnp
from jax import lax
from jax.experimental import pallas as pl
from jax.experimental.pallas import tpu as pltpu
from jax.sharding import PartitionSpec as P

HEAD_SIZE = 128
MESH = pl.DeviceIdType.MESH
F32 = jnp.float32
BF16 = jnp.bfloat16
SPLIT = 2


def dot(a, b, ca, cb):
    return lax.dot_general(a, b, (((ca,), (cb,)), ((), ())), preferred_element_type=F32)


def kernel(
    nd, total_entries,
    x_in, q_in, k_in, v_in, do_in, wq_ref, wk_ref, wv_ref, mq_ref, mk_ref, mv_ref,
    dx_out, vq_out, vk_out, vv_out,
    g_all, x_all, w_cat, acc, part, fpart, p_buf, y_buf, d_buf, ws, wr, sq, mq, mk, mv,
    x_ref, q_ref, k_ref, v_ref, do_ref, dx_ref,
    xs_s, xs_r, xy_s, xy_r, w_s, w_r, col_s, col_r, re_s, re_r, fd_s, fd_r, xn_s, xn_r, dd_s, dd_r,
    py_s, py_r, dx_s, dx_r, dw_s, dw_r, sq_s, sq_r, m_s, in_s, win_s, dxo_s, vo_s,
):
    kv = g_all.shape[0]
    group = g_all.shape[1]
    half = g_all.shape[3]
    seq = 2 * half
    wide = g_all.shape[4]
    grp = q_ref.shape[2] // k_ref.shape[2]
    gq = grp * HEAD_SIZE
    rows = wq_ref.shape[0]
    sub = half // SPLIT
    near = group // 2
    nz = nd // 4
    d = lax.axis_index("dp")
    t = lax.axis_index("tensor")
    c = d % 2
    xx = (d // 2) % 2
    z = d // 4

    def other_half(e):
        return e + 4 * (1 - 2 * ((e // 4) % 2))

    def member(r):
        zr = nz - 1 - z if r & 4 else z
        xr = 1 - xx if r & 2 else xx
        cr = 1 - c if r & 1 else c
        return (zr * 2 + xr) * 2 + cr

    def columns(e):
        return pl.ds(pl.multiple_of(e * rows, 128), rows)

    def to(dp, tt):
        return {"dp": dp, "tensor": tt}

    def rcopy(src, dst, ss, rs, dev):
        return pltpu.make_async_remote_copy(
            src_ref=src, dst_ref=dst, send_sem=ss, recv_sem=rs, device_id=dev, device_id_type=MESH
        )

    far = other_half(d)
    outer = jnp.logical_or(z == 0, z == nz - 1)
    inner = jnp.logical_not(outer)
    me = d * 2 + t
    total_devices = nd * 2
    bar = pltpu.get_barrier_semaphore()

    for e in [member(r) for r in range(1, group)] + [far]:
        pl.semaphore_signal(bar, inc=1, device_id=to(e, t), device_id_type=MESH)
    pl.semaphore_signal(bar, inc=1, device_id=to(d, 1 - t), device_id_type=MESH)
    pieces = []
    for j in range(kv):
        cq = slice(j * gq, (j + 1) * gq)
        ck = slice(j * HEAD_SIZE, (j + 1) * HEAD_SIZE)
        for i, (src, cut, lo, hi) in enumerate((
            (wq_ref, cq, 0, gq), (wk_ref, ck, gq, gq + HEAD_SIZE), (wv_ref, ck, gq + HEAD_SIZE, wide)
        )):
            pieces.append(
                pltpu.make_async_copy(src.at[:, cut], w_cat.at[j, 0:rows, lo:hi], win_s.at[j, i])
            )
    loads = [
        pltpu.make_async_copy(src, dst, in_s.at[i])
        for i, (src, dst) in enumerate(
            ((x_in, x_ref), (k_in, k_ref), (q_in, q_ref), (v_in, v_ref), (do_in, do_ref))
        )
    ]
    for copy in (loads[0], *pieces, *loads[1:]):
        copy.start()
    momentum = [
        pltpu.make_async_copy(src, dst, m_s.at[i])
        for i, (src, dst) in enumerate(((mq_ref, mq), (mk_ref, mk), (mv_ref, mv)))
    ]
    for copy in momentum:
        copy.start()

    for copy in (loads[0], *pieces):
        copy.wait()
    pl.semaphore_wait(bar, group + 1)

    def xcopy(r, f):
        e = member(r)
        src = e if f == 0 else other_half(e)
        return rcopy(
            x_ref.at[0, :, columns(src)], x_all.at[r, t, :, f * rows:(f + 1) * rows],
            xs_s.at[r, f], xs_r.at[r, f], to(e, t),
        )

    def xfwd(r):
        return rcopy(x_all.at[r, t], x_all.at[r, t], xy_s.at[r], xy_r.at[r], to(d, 1 - t))

    def xfwd_wait(r):
        rcopy(x_all.at[r, 1 - t], x_all.at[r, 1 - t], xy_s.at[r], xy_r.at[r], to(d, 1 - t)).wait_recv()

    def wcopy(j):
        return rcopy(
            w_cat.at[j, 0:rows], w_cat.at[j, rows:2 * rows], w_s.at[j], w_r.at[j], to(far, t)
        )

    def piece(j, r, h):
        return g_all.at[j, r, :, pl.ds(pl.multiple_of(h * sub, sub), sub)]

    def colcopy(h, j):
        return rcopy(
            piece(j, 0, h), piece(j, 4, h), col_s.at[h, j], col_r.at[h, j], to(member(4), t)
        )

    def relay(h, j):
        return rcopy(
            piece(j, 4, h), piece(j, 6, h), re_s.at[h, j], re_r.at[h, j], to(member(2), t)
        )

    def fardd(i, h, j):
        return rcopy(
            piece(j, 4 + 2 * i, h), piece(j, 5 + 2 * i, h),
            fd_s.at[i, h, j], fd_r.at[i, h, j], to(member(1), t),
        )

    def xncopy(j):
        return rcopy(g_all.at[j, 0], g_all.at[j, 2], xn_s.at[j], xn_r.at[j], to(member(2), t))

    def ddcopy(i, j):
        return rcopy(
            g_all.at[j, 2 * i], g_all.at[j, 2 * i + 1], dd_s.at[i, j], dd_r.at[i, j], to(member(1), t)
        )

    for j in range(kv):
        wcopy(j).start()
    for r in (4, 5, 6, 7, 2, 3, 1):
        for f in range(2):
            xcopy(r, f).start()
    for f, e in ((0, d), (1, far)):
        x_all[0, t, :, f * rows:(f + 1) * rows] = x_ref[0, :, columns(e)]
    xfwd(0).start()

    for copy in loads[1:]:
        copy.wait()
    scaling = 1.0 / math.sqrt(HEAD_SIZE)

    def attention(j, _):
        kk = k_ref[0, :, pl.ds(pl.multiple_of(j * HEAD_SIZE, 128), HEAD_SIZE)]
        vv = v_ref[0, :, pl.ds(pl.multiple_of(j * HEAD_SIZE, 128), HEAD_SIZE)]
        dk = jnp.zeros((seq, HEAD_SIZE), F32)
        dv = jnp.zeros((seq, HEAD_SIZE), F32)
        mask = lax.broadcasted_iota(jnp.int32, (seq, seq), 0) >= lax.broadcasted_iota(
            jnp.int32, (seq, seq), 1
        )
        for g in range(grp):
            cols = pl.ds(pl.multiple_of(j * gq + g * HEAD_SIZE, 128), HEAD_SIZE)
            qq = q_ref[0, :, cols]
            oo = do_ref[0, :, cols]
            s = jnp.where(mask, dot(qq, kk, 1, 1) * scaling, -jnp.inf)
            e = jnp.exp(s - jnp.max(s, axis=-1, keepdims=True))
            soft = e / jnp.sum(e, axis=-1, keepdims=True)
            gs = dot(oo, vv, 1, 1)
            delta = jnp.sum(soft * gs, axis=-1, keepdims=True)
            ds = (soft * (gs - delta) * scaling).astype(BF16)
            g_all[j, 0, :, :, g * HEAD_SIZE:(g + 1) * HEAD_SIZE] = (
                dot(ds, kk, 1, 0).astype(BF16).reshape(2, half, HEAD_SIZE)
            )
            dk = dk + dot(ds, qq, 0, 0)
            dv = dv + dot(soft.astype(BF16), oo, 0, 0)
        g_all[j, 0, :, :, gq:gq + HEAD_SIZE] = dk.astype(BF16).reshape(2, half, HEAD_SIZE)
        g_all[j, 0, :, :, gq + HEAD_SIZE:wide] = dv.astype(BF16).reshape(2, half, HEAD_SIZE)
        colcopy(0, j).start()

        @pl.when(jnp.logical_and(inner, j % 2 == 1))
        def _():
            for h in range(1, SPLIT):
                colcopy(h, j - 1).start()
                colcopy(h, j).start()

        xncopy(j).start()
        ddcopy(0, j).start()
        return 0

    lax.fori_loop(0, kv, attention, 0)

    @pl.when(outer)
    def _():
        for h in range(1, SPLIT):
            for j in range(kv):
                colcopy(h, j).start()

    def xready(r):
        for f in range(2):
            xcopy(r, f).wait_recv()
        xfwd(r).start()

    for r in range(1, group):
        xready(r)

    for r in range(group):
        xfwd_wait(r)

    steps = SPLIT * kv

    def pcopy(r, h):
        span = pl.ds(pl.multiple_of(h * sub, sub), sub)
        return rcopy(
            p_buf.at[r, 1 - t, span], y_buf.at[r, span], py_s.at[r, h], py_r.at[r, h], to(d, 1 - t)
        )

    def dxcopy(r, f, h, e):
        span = pl.ds(pl.multiple_of(h * sub, sub), sub)
        return rcopy(
            d_buf.at[r, span, f * rows:(f + 1) * rows], dx_ref.at[0, span, columns(e)],
            dx_s.at[r, f, h], dx_r.at[r, f, h], to(member(r), t),
        )

    def finish(r, h):
        span = pl.ds(pl.multiple_of(h * sub, sub), sub)
        pcopy(r, h).wait_recv()
        total = (p_buf[r, t, span].astype(F32) + y_buf[r, span].astype(F32)).astype(BF16)
        if r == 0:
            for f, e in ((0, d), (1, far)):
                dx_ref[0, span, columns(e)] = total[:, f * rows:(f + 1) * rows]
        else:
            d_buf[r, span] = total
            for f, e in ((0, d), (1, far)):
                dxcopy(r, f, h, e).start()

    def dwcopy(j):
        return rcopy(ws.at[j], wr.at[j], dw_s.at[j], dw_r.at[j], to(far, t))

    def place(i):
        h = jnp.where(outer, i // kv, (i % (2 * SPLIT)) // 2)
        return h, jnp.where(outer, i % kv, 2 * (i // (2 * SPLIT)) + i % 2)

    def receive(i):
        h, j = place(i)
        colcopy(h, j).wait_recv()
        relay(h, j).start()
        fardd(0, h, j).start()

        @pl.when(i < kv)
        def _():
            xncopy(i).wait_recv()
            ddcopy(1, i).start()

    def close(j):
        ddcopy(0, j).wait_recv()
        ddcopy(1, j).wait_recv()
        wcopy(j).wait_recv()
        gs = g_all[j, 0:near].reshape(near * seq, wide)
        acc[j] = dot(x_all[0:near].reshape(near * seq, 2 * rows), gs, 0, 0)
        new = dot(gs, w_cat[j], 1, 1)

        @pl.when(j == 0)
        def _():
            part[...] = new

        @pl.when(j > 0)
        def _():
            part[...] += new

    def distant(i):
        h, j = place(i)
        span = pl.ds(pl.multiple_of(h * sub, sub), sub)
        relay(h, j).wait_recv()
        fardd(1, h, j).start()

        fardd(0, h, j).wait_recv()
        fardd(1, h, j).wait_recv()
        gs = g_all[j, near:group, :, span].reshape(near * 2 * sub, wide)
        acc[j] += dot(x_all[near:group, :, span].reshape(near * 2 * sub, 2 * rows), gs, 0, 0)

        @pl.when(h == SPLIT - 1)
        def _():
            ws[j] = acc[j, rows:2 * rows].astype(BF16)
            dwcopy(j).start()

        new = dot(gs, w_cat[j], 1, 1)

        @pl.when(j == 0)
        def _():
            fpart[h] = new

        @pl.when(j > 0)
        def _():
            fpart[h] += new

        @pl.when(j == kv - 1)
        def _():
            for r in range(near, group):
                lo = (r - near) * 2 * sub
                p_buf[r, :, span] = (
                    fpart[h, lo:lo + 2 * sub].astype(BF16).reshape(2, sub, 2 * rows)
                )
                pcopy(r, h).start()

    def step(i, _):
        @pl.when(i < steps)
        def _():
            receive(i)

        @pl.when(jnp.logical_and(i > 0, i <= kv))
        def _():
            close(i - 1)

        @pl.when(i > 0)
        def _():
            distant(i - 1)

        @pl.when(i == kv)
        def _():
            for r in range(near):
                p_buf[r] = part[r * seq:(r + 1) * seq].astype(BF16).reshape(2, half, 2 * rows)
                for h in range(SPLIT):
                    pcopy(r, h).start()

        @pl.when(i == jnp.where(outer, kv + 2, steps))
        def _():
            for r in range(near, group):
                finish(r, 0)

        return 0

    lax.fori_loop(0, steps + 1, step, 0)
    for h in range(1, SPLIT):
        for r in range(near, group):
            finish(r, h)
    for r in range(near):
        for h in range(SPLIT):
            finish(r, h)

    squares = jnp.zeros((1, 1), F32)
    for j in range(kv):
        dwcopy(j).wait_recv()
        a = acc[j, 0:rows] + wr[j].astype(F32)
        acc[j, 0:rows] = a
        squares = squares + jnp.sum(a * a, keepdims=True)
    sq[me] = jnp.broadcast_to(squares, (1, 128))

    def sqcopy(e, slot):
        return rcopy(sq.at[slot], sq.at[slot], sq_s.at[e], sq_r.at[slot], to(e // 2, e % 2))

    def sqsend(i, _):
        sqcopy((me + i) % total_devices, me).start()
        return 0

    lax.fori_loop(1, total_devices, sqsend, 0)

    for r in range(1, group):
        e = member(r)
        for f in range(2):
            xcopy(r, f).wait_send()
            for h in range(SPLIT):
                dxcopy(r, f, h, d).wait_send()
                dxcopy(r, f, h, e if f == 0 else other_half(e)).wait_recv()
    dx_store = pltpu.make_async_copy(dx_ref, dx_out, dxo_s)
    dx_store.start()
    for r in range(group):
        xfwd(r).wait_send()
        for h in range(SPLIT):
            pcopy(r, h).wait_send()

    def drain_g(j, _):
        wcopy(j).wait_send()
        dwcopy(j).wait_send()
        xncopy(j).wait_send()
        for i in range(2):
            ddcopy(i, j).wait_send()
        for h in range(SPLIT):
            colcopy(h, j).wait_send()
            relay(h, j).wait_send()
            for i in range(2):
                fardd(i, h, j).wait_send()
        return 0

    lax.fori_loop(0, kv, drain_g, 0)

    def drain(i, _):
        e = (me + i) % total_devices
        sqcopy(e, me).wait_send()
        sqcopy(e, e).wait_recv()
        return 0

    lax.fori_loop(1, total_devices, drain, 0)
    total = jnp.sum(sq[...], axis=0)[0:1, 0:1]
    factor = 1.0 / jnp.maximum(jnp.sqrt(total / total_entries), 1.0)
    for copy in momentum:
        copy.wait()
    stores = []
    for j in range(kv):
        cq = slice(j * gq, (j + 1) * gq)
        ck = slice(j * HEAD_SIZE, (j + 1) * HEAD_SIZE)
        for i, (buf, dst, cut, lo, hi) in enumerate((
            (mq, vq_out, cq, 0, gq),
            (mk, vk_out, ck, gq, gq + HEAD_SIZE),
            (mv, vv_out, ck, gq + HEAD_SIZE, wide),
        )):
            buf[:, cut] = 0.9 * buf[:, cut] + factor * acc[j, 0:rows, lo:hi]
            stores.append(pltpu.make_async_copy(buf.at[:, cut], dst.at[:, cut], vo_s.at[j, i]))
            stores[-1].start()
    for copy in (dx_store, *stores):
        copy.wait()


def fused(nd, nt, inputs, q, k, v, do, wq, wk, wv, mq, mk, mv):
    seq = q.shape[1]
    kv = k.shape[2] // HEAD_SIZE
    wide = (q.shape[2] + 2 * k.shape[2]) // kv
    rows = wq.shape[0]
    half = seq // nt
    group = nd // 2
    total_entries = float(rows * nd * kv * wide * nt)
    dma = pltpu.SemaphoreType.DMA
    return pl.pallas_call(
        functools.partial(kernel, nd, total_entries),
        out_shape=(
            jax.ShapeDtypeStruct(inputs.shape, BF16),
            jax.ShapeDtypeStruct(wq.shape, F32),
            jax.ShapeDtypeStruct(wk.shape, F32),
            jax.ShapeDtypeStruct(wv.shape, F32),
        ),
        in_specs=[pl.BlockSpec(memory_space=pltpu.HBM)] * 11,
        out_specs=(pl.BlockSpec(memory_space=pltpu.HBM),) * 4,
        scratch_shapes=[
            pltpu.VMEM((kv, group, nt, half, wide), BF16),
            pltpu.VMEM((group, nt, half, 2 * rows), BF16),
            pltpu.VMEM((kv, 2 * rows, wide), BF16),
            pltpu.VMEM((kv, 2 * rows, wide), F32),
            pltpu.VMEM((group // 2 * seq, 2 * rows), F32),
            pltpu.VMEM((SPLIT, group // 2 * seq // SPLIT, 2 * rows), F32),
            pltpu.VMEM((group, nt, half, 2 * rows), BF16),
            pltpu.VMEM((group, half, 2 * rows), BF16),
            pltpu.VMEM((group, half, 2 * rows), BF16),
            pltpu.VMEM((kv, rows, wide), BF16),
            pltpu.VMEM((kv, rows, wide), BF16),
            pltpu.VMEM((nd * nt, 1, 128), F32),
            pltpu.VMEM(mq.shape, F32),
            pltpu.VMEM(mk.shape, F32),
            pltpu.VMEM(mv.shape, F32),
            pltpu.VMEM(inputs.shape, BF16),
            pltpu.VMEM(q.shape, BF16),
            pltpu.VMEM(k.shape, BF16),
            pltpu.VMEM(v.shape, BF16),
            pltpu.VMEM(do.shape, BF16),
            pltpu.VMEM(inputs.shape, BF16),
            dma((group, 2)), dma((group, 2)), dma((group,)), dma((group,)),
            dma((kv,)), dma((kv,)), dma((SPLIT, kv)), dma((SPLIT, kv)),
            dma((SPLIT, kv)), dma((SPLIT, kv)), dma((2, SPLIT, kv)), dma((2, SPLIT, kv)),
            dma((kv,)), dma((kv,)), dma((2, kv)), dma((2, kv)),
            dma((group, SPLIT)), dma((group, SPLIT)), dma((group, 2, SPLIT)), dma((group, 2, SPLIT)),
            dma((kv,)), dma((kv,)), dma((nd * nt,)), dma((nd * nt,)), dma((3,)), dma((5,)), dma((kv, 3)), dma, dma((kv, 3)),
        ],
        compiler_params=pltpu.CompilerParams(
            collective_id=0, has_side_effects=True, vmem_limit_bytes=60 * 1024 * 1024
        ),
    )(inputs, q, k, v, do, wq, wk, wv, mq, mk, mv)


def pieces_of(shape):
    axis = len(shape) - 2
    step = shape[axis] // 2
    return [(slice(None),) * axis + (slice(i * step, (i + 1) * step),) for i in range(2)]


def hand_kernel(*refs):
    ins, outs, bufs, (get_s, put_s) = refs[0:4], refs[4:8], refs[8:12], refs[12:14]
    gets, puts = [], []
    for i in range(4):
        for k, cut in enumerate(pieces_of(ins[i].shape)):
            gets.append(pltpu.make_async_copy(ins[i].at[cut], bufs[i].at[cut], get_s.at[i, k]))
            puts.append(pltpu.make_async_copy(bufs[i].at[cut], outs[i].at[cut], put_s.at[i, k]))
    for get in gets:
        get.start()
    for get, put in zip(gets, puts):
        get.wait()
        put.start()
    for put in puts:
        put.wait()


def handed(*arrays):
    hbm = pl.BlockSpec(memory_space=pltpu.HBM)
    return pl.pallas_call(
        hand_kernel,
        out_shape=tuple(jax.ShapeDtypeStruct(a.shape, a.dtype) for a in arrays),
        in_specs=[hbm] * 4,
        out_specs=(hbm,) * 4,
        scratch_shapes=[pltpu.VMEM(a.shape, a.dtype) for a in arrays]
        + [pltpu.SemaphoreType.DMA((4, 2))] * 2,
        compiler_params=pltpu.CompilerParams(vmem_limit_bytes=60 * 1024 * 1024),
    )(*arrays)


def heads_backward(query_row_set, key_rows, value_rows, cotangent_rows):
    token_length = query_row_set.shape[0]
    kv_heads = key_rows.shape[1] // HEAD_SIZE
    group_width = query_row_set.shape[1] // HEAD_SIZE // kv_heads
    scaling = 1.0 / math.sqrt(HEAD_SIZE)
    query_quad = query_row_set.reshape(token_length, kv_heads, group_width, HEAD_SIZE)
    cotangent_quad = cotangent_rows.reshape(token_length, kv_heads, group_width, HEAD_SIZE)
    key_triple = key_rows.reshape(token_length, kv_heads, HEAD_SIZE)
    value_triple = value_rows.reshape(token_length, kv_heads, HEAD_SIZE)
    block_rows = min(token_length, 512)
    key_sums = jnp.zeros((token_length, kv_heads, HEAD_SIZE), F32)
    value_sums = jnp.zeros((token_length, kv_heads, HEAD_SIZE), F32)
    query_blocks = []
    for row_start in range(0, token_length, block_rows):
        row_end = row_start + block_rows
        query_block = query_quad[row_start:row_end]
        cotangent_block = cotangent_quad[row_start:row_end]
        key_block = key_triple[:row_end]
        value_block = value_triple[:row_end]
        scores = (
            jnp.einsum("ihgd,jhd->hgij", query_block, key_block, preferred_element_type=F32)
            * scaling
        )
        query_index = row_start + lax.broadcasted_iota(jnp.int32, (block_rows, row_end), 0)
        key_index = lax.broadcasted_iota(jnp.int32, (block_rows, row_end), 1)
        scores = jnp.where(query_index >= key_index, scores, -jnp.inf)
        maximum = jnp.max(scores, axis=-1, keepdims=True)
        exponent = jnp.exp(scores - maximum)
        softmax_rows = exponent / jnp.sum(exponent, axis=-1, keepdims=True)
        softmax_reduced = softmax_rows.astype(BF16)
        grad_softmax = jnp.einsum(
            "ihgd,jhd->hgij", cotangent_block, value_block, preferred_element_type=F32
        )
        row_delta = jnp.sum(softmax_rows * grad_softmax, axis=-1, keepdims=True)
        score_gradient = (softmax_rows * (grad_softmax - row_delta) * scaling).astype(BF16)
        query_blocks.append(
            jnp.einsum(
                "hgij,jhd->ihgd", score_gradient, key_block, preferred_element_type=F32
            ).astype(BF16)
        )
        key_sums = key_sums.at[:row_end].add(
            jnp.einsum(
                "xfwo,wxfp->oxp", score_gradient, query_block, preferred_element_type=F32
            )
        )
        value_sums = value_sums.at[:row_end].add(
            jnp.einsum(
                "xfwo,wxfp->oxp",
                softmax_reduced,
                cotangent_block,
                preferred_element_type=F32,
            )
        )
    grad_query = jnp.concatenate(query_blocks, axis=0).reshape(token_length, -1)
    key_gradient = key_sums.astype(BF16).reshape(token_length, -1)
    value_gradient = value_sums.astype(BF16).reshape(token_length, -1)
    return (grad_query, key_gradient, value_gradient)


def small(nd, nt, inputs, query_states, key_states, query_weight):
    seq = query_states.shape[1]
    cols = query_states.shape[2] + 2 * key_states.shape[2]
    held = nd * seq * cols * 2 + 10 * nd * seq * query_weight.shape[0]
    even = key_states.shape[2] % (2 * HEAD_SIZE) == 0
    return nt == 2 and nd == 16 and even and held < 36 * 1024 * 1024


def local(nd, nt, *args):
    inputs, q, k, v, do, wq, wk, wv, mq, mk, mv = args
    if small(nd, nt, inputs, q, k, wq):
        return handed(*fused(nd, nt, *args))
    else:
        query_cols = wq.shape[1]
        pair_cols = wk.shape[1]
        rows = wq.shape[0]
        weights = jnp.concatenate((wq, wk, wv), axis=1)
        grads = jnp.concatenate(heads_backward(q[0], k[0], v[0], do[0]), axis=1)
        all_grads = lax.all_gather(grads, "dp", axis=0, tiled=True)
        pieces = lax.all_to_all(inputs[0], "dp", 1, 0, tiled=True)
        pieces = pieces.reshape(nd, -1, rows)
        all_inputs = lax.all_gather(pieces, "tensor", axis=1, tiled=True).reshape(-1, rows)
        summed = dot(all_inputs, all_grads, 0, 0)
        parts = dot(all_grads, weights, 1, 1).astype(BF16).reshape(nd, -1, rows)
        mine = lax.psum_scatter(parts, "tensor", scatter_dimension=1, tiled=True)
        grad_inputs = lax.all_to_all(mine.reshape(-1, rows), "dp", 0, 1, tiled=True)[None]
        total = lax.psum(jnp.sum(summed * summed), ("dp", "tensor"))
        factor = 1.0 / jnp.maximum(jnp.sqrt(total / (summed.size * nd * nt)), 1.0)
        gq = summed[:, :query_cols]
        gk = summed[:, query_cols:query_cols + pair_cols]
        gv = summed[:, query_cols + pair_cols:]
    return (
        grad_inputs,
        0.9 * mq + factor * gq,
        0.9 * mk + factor * gk,
        0.9 * mv + factor * gv,
    )


def solution(mesh):
    nd, nt = mesh.shape["dp"], mesh.shape["tensor"]
    saved = P("dp", None, "tensor")
    tokens = P("dp", "tensor", None)
    weight = P("dp", "tensor")
    return jax.shard_map(
        functools.partial(local, nd, nt),
        mesh=mesh,
        in_specs=(tokens,) + (saved,) * 4 + (weight,) * 6,
        out_specs=(tokens,) + (weight,) * 3,
        check_vma=False,
    )
```

```python
import functools
import math

import jax
import jax.numpy as jnp
from jax import lax
from jax.experimental import pallas as pl
from jax.experimental.pallas import tpu as pltpu
from jax.sharding import PartitionSpec as P

HEAD_SIZE = 128
MESH = pl.DeviceIdType.MESH
F32 = jnp.float32
BF16 = jnp.bfloat16
SPLIT = 2


def dot(a, b, ca, cb):
    return lax.dot_general(a, b, (((ca,), (cb,)), ((), ())), preferred_element_type=F32)


def kernel(
    nd, total_entries,
    x_in, q_in, k_in, v_in, do_in, wq_ref, wk_ref, wv_ref, mq_ref, mk_ref, mv_ref,
    dx_out, vq_out, vk_out, vv_out,
    g_all, x_all, w_cat, acc, part, fpart, p_buf, y_buf, d_buf, ws, wr, sq, mq, mk, mv,
    x_ref, q_ref, k_ref, v_ref, do_ref, dx_ref,
    xs_s, xs_r, xy_s, xy_r, w_s, w_r, col_s, col_r, re_s, re_r, fd_s, fd_r, xn_s, xn_r, dd_s, dd_r,
    py_s, py_r, dx_s, dx_r, dw_s, dw_r, sq_s, sq_r, m_s, in_s, win_s, dxo_s, vo_s,
):
    kv = g_all.shape[0]
    group = g_all.shape[1]
    half = g_all.shape[3]
    seq = 2 * half
    wide = g_all.shape[4]
    grp = q_ref.shape[2] // k_ref.shape[2]
    gq = grp * HEAD_SIZE
    rows = wq_ref.shape[0]
    sub = half // SPLIT
    near = group // 2
    nz = nd // 4
    d = lax.axis_index("dp")
    t = lax.axis_index("tensor")
    c = d % 2
    xx = (d // 2) % 2
    z = d // 4

    def other_half(e):
        return e + 4 * (1 - 2 * ((e // 4) % 2))

    def member(r):
        zr = nz - 1 - z if r & 4 else z
        xr = 1 - xx if r & 2 else xx
        cr = 1 - c if r & 1 else c
        return (zr * 2 + xr) * 2 + cr

    def columns(e):
        return pl.ds(pl.multiple_of(e * rows, 128), rows)

    def to(dp, tt):
        return {"dp": dp, "tensor": tt}

    def rcopy(src, dst, ss, rs, dev):
        return pltpu.make_async_remote_copy(
            src_ref=src, dst_ref=dst, send_sem=ss, recv_sem=rs, device_id=dev, device_id_type=MESH
        )

    far = other_half(d)
    outer = jnp.logical_or(z == 0, z == nz - 1)
    inner = jnp.logical_not(outer)
    me = d * 2 + t
    total_devices = nd * 2
    bar = pltpu.get_barrier_semaphore()

    for e in [member(r) for r in range(1, group)] + [far]:
        pl.semaphore_signal(bar, inc=1, device_id=to(e, t), device_id_type=MESH)
    pl.semaphore_signal(bar, inc=1, device_id=to(d, 1 - t), device_id_type=MESH)
    pieces = []
    for j in range(kv):
        cq = slice(j * gq, (j + 1) * gq)
        ck = slice(j * HEAD_SIZE, (j + 1) * HEAD_SIZE)
        for i, (src, cut, lo, hi) in enumerate((
            (wq_ref, cq, 0, gq), (wk_ref, ck, gq, gq + HEAD_SIZE), (wv_ref, ck, gq + HEAD_SIZE, wide)
        )):
            pieces.append(
                pltpu.make_async_copy(src.at[:, cut], w_cat.at[j, 0:rows, lo:hi], win_s.at[j, i])
            )
    loads = [
        pltpu.make_async_copy(src, dst, in_s.at[i])
        for i, (src, dst) in enumerate(
            ((x_in, x_ref), (k_in, k_ref), (q_in, q_ref), (v_in, v_ref), (do_in, do_ref))
        )
    ]
    for copy in (loads[0], *pieces, *loads[1:]):
        copy.start()
    momentum = [
        pltpu.make_async_copy(src, dst, m_s.at[i])
        for i, (src, dst) in enumerate(((mq_ref, mq), (mk_ref, mk), (mv_ref, mv)))
    ]
    for copy in momentum:
        copy.start()

    for copy in (loads[0], *pieces):
        copy.wait()
    pl.semaphore_wait(bar, group + 1)

    def xcopy(r, f):
        e = member(r)
        src = e if f == 0 else other_half(e)
        return rcopy(
            x_ref.at[0, :, columns(src)], x_all.at[r, t, :, f * rows:(f + 1) * rows],
            xs_s.at[r, f], xs_r.at[r, f], to(e, t),
        )

    def xfwd(r):
        return rcopy(x_all.at[r, t], x_all.at[r, t], xy_s.at[r], xy_r.at[r], to(d, 1 - t))

    def xfwd_wait(r):
        rcopy(x_all.at[r, 1 - t], x_all.at[r, 1 - t], xy_s.at[r], xy_r.at[r], to(d, 1 - t)).wait_recv()

    def wcopy(j):
        return rcopy(
            w_cat.at[j, 0:rows], w_cat.at[j, rows:2 * rows], w_s.at[j], w_r.at[j], to(far, t)
        )

    def piece(j, r, h):
        return g_all.at[j, r, :, pl.ds(pl.multiple_of(h * sub, sub), sub)]

    def colcopy(h, j):
        return rcopy(
            piece(j, 0, h), piece(j, 4, h), col_s.at[h, j], col_r.at[h, j], to(member(4), t)
        )

    def relay(h, j):
        return rcopy(
            piece(j, 4, h), piece(j, 6, h), re_s.at[h, j], re_r.at[h, j], to(member(2), t)
        )

    def fardd(i, h, j):
        return rcopy(
            piece(j, 4 + 2 * i, h), piece(j, 5 + 2 * i, h),
            fd_s.at[i, h, j], fd_r.at[i, h, j], to(member(1), t),
        )

    def xncopy(j):
        return rcopy(g_all.at[j, 0], g_all.at[j, 2], xn_s.at[j], xn_r.at[j], to(member(2), t))

    def ddcopy(i, j):
        return rcopy(
            g_all.at[j, 2 * i], g_all.at[j, 2 * i + 1], dd_s.at[i, j], dd_r.at[i, j], to(member(1), t)
        )

    for j in range(kv):
        wcopy(j).start()
    for r in (4, 5, 6, 7, 2, 3, 1):
        for f in range(2):
            xcopy(r, f).start()
    for f, e in ((0, d), (1, far)):
        x_all[0, t, :, f * rows:(f + 1) * rows] = x_ref[0, :, columns(e)]
    xfwd(0).start()

    for copy in loads[1:]:
        copy.wait()
    scaling = 1.0 / math.sqrt(HEAD_SIZE)

    def attention(j, _):
        kk = k_ref[0, :, pl.ds(pl.multiple_of(j * HEAD_SIZE, 128), HEAD_SIZE)]
        vv = v_ref[0, :, pl.ds(pl.multiple_of(j * HEAD_SIZE, 128), HEAD_SIZE)]
        dk = jnp.zeros((seq, HEAD_SIZE), F32)
        dv = jnp.zeros((seq, HEAD_SIZE), F32)
        mask = lax.broadcasted_iota(jnp.int32, (seq, seq), 0) >= lax.broadcasted_iota(
            jnp.int32, (seq, seq), 1
        )
        for g in range(grp):
            cols = pl.ds(pl.multiple_of(j * gq + g * HEAD_SIZE, 128), HEAD_SIZE)
            qq = q_ref[0, :, cols]
            oo = do_ref[0, :, cols]
            s = jnp.where(mask, dot(qq, kk, 1, 1) * scaling, -jnp.inf)
            e = jnp.exp(s - jnp.max(s, axis=-1, keepdims=True))
            soft = e / jnp.sum(e, axis=-1, keepdims=True)
            gs = dot(oo, vv, 1, 1)
            delta = jnp.sum(soft * gs, axis=-1, keepdims=True)
            ds = (soft * (gs - delta) * scaling).astype(BF16)
            g_all[j, 0, :, :, g * HEAD_SIZE:(g + 1) * HEAD_SIZE] = (
                dot(ds, kk, 1, 0).astype(BF16).reshape(2, half, HEAD_SIZE)
            )
            dk = dk + dot(ds, qq, 0, 0)
            dv = dv + dot(soft.astype(BF16), oo, 0, 0)
        g_all[j, 0, :, :, gq:gq + HEAD_SIZE] = dk.astype(BF16).reshape(2, half, HEAD_SIZE)
        g_all[j, 0, :, :, gq + HEAD_SIZE:wide] = dv.astype(BF16).reshape(2, half, HEAD_SIZE)
        colcopy(0, j).start()

        @pl.when(jnp.logical_and(inner, j % 2 == 1))
        def _():
            for h in range(1, SPLIT):
                colcopy(h, j - 1).start()
                colcopy(h, j).start()

        xncopy(j).start()
        ddcopy(0, j).start()
        return 0

    lax.fori_loop(0, kv, attention, 0)

    @pl.when(outer)
    def _():
        for h in range(1, SPLIT):
            for j in range(kv):
                colcopy(h, j).start()

    def xready(r):
        for f in range(2):
            xcopy(r, f).wait_recv()
        xfwd(r).start()

    for r in range(1, group):
        xready(r)

    for r in range(group):
        xfwd_wait(r)

    steps = SPLIT * kv

    def pcopy(r, h):
        span = pl.ds(pl.multiple_of(h * sub, sub), sub)
        return rcopy(
            p_buf.at[r, 1 - t, span], y_buf.at[r, span], py_s.at[r, h], py_r.at[r, h], to(d, 1 - t)
        )

    def dxcopy(r, f, h, e):
        span = pl.ds(pl.multiple_of(h * sub, sub), sub)
        return rcopy(
            d_buf.at[r, span, f * rows:(f + 1) * rows], dx_ref.at[0, span, columns(e)],
            dx_s.at[r, f, h], dx_r.at[r, f, h], to(member(r), t),
        )

    def finish(r, h):
        span = pl.ds(pl.multiple_of(h * sub, sub), sub)
        pcopy(r, h).wait_recv()
        total = (p_buf[r, t, span].astype(F32) + y_buf[r, span].astype(F32)).astype(BF16)
        if r == 0:
            for f, e in ((0, d), (1, far)):
                dx_ref[0, span, columns(e)] = total[:, f * rows:(f + 1) * rows]
        else:
            d_buf[r, span] = total
            for f, e in ((0, d), (1, far)):
                dxcopy(r, f, h, e).start()

    def dwcopy(j):
        return rcopy(ws.at[j], wr.at[j], dw_s.at[j], dw_r.at[j], to(far, t))

    def place(i):
        h = jnp.where(outer, i // kv, (i % (2 * SPLIT)) // 2)
        return h, jnp.where(outer, i % kv, 2 * (i // (2 * SPLIT)) + i % 2)

    def receive(i):
        h, j = place(i)
        colcopy(h, j).wait_recv()
        relay(h, j).start()
        fardd(0, h, j).start()

        @pl.when(i < kv)
        def _():
            xncopy(i).wait_recv()
            ddcopy(1, i).start()

    def close(j):
        ddcopy(0, j).wait_recv()
        ddcopy(1, j).wait_recv()
        wcopy(j).wait_recv()
        gs = g_all[j, 0:near].reshape(near * seq, wide)
        acc[j] = dot(x_all[0:near].reshape(near * seq, 2 * rows), gs, 0, 0)
        new = dot(gs, w_cat[j], 1, 1)

        @pl.when(j == 0)
        def _():
            part[...] = new

        @pl.when(j > 0)
        def _():
            part[...] += new

    def distant(i):
        h, j = place(i)
        span = pl.ds(pl.multiple_of(h * sub, sub), sub)
        relay(h, j).wait_recv()
        fardd(1, h, j).start()

        fardd(0, h, j).wait_recv()
        fardd(1, h, j).wait_recv()
        gs = g_all[j, near:group, :, span].reshape(near * 2 * sub, wide)
        acc[j] += dot(x_all[near:group, :, span].reshape(near * 2 * sub, 2 * rows), gs, 0, 0)

        @pl.when(h == SPLIT - 1)
        def _():
            ws[j] = acc[j, rows:2 * rows].astype(BF16)
            dwcopy(j).start()

        new = dot(gs, w_cat[j], 1, 1)

        @pl.when(j == 0)
        def _():
            fpart[h] = new

        @pl.when(j > 0)
        def _():
            fpart[h] += new

        @pl.when(j == kv - 1)
        def _():
            for r in range(near, group):
                lo = (r - near) * 2 * sub
                p_buf[r, :, span] = (
                    fpart[h, lo:lo + 2 * sub].astype(BF16).reshape(2, sub, 2 * rows)
                )
                pcopy(r, h).start()

    def step(i, _):
        @pl.when(i < steps)
        def _():
            receive(i)

        @pl.when(jnp.logical_and(i > 0, i <= kv))
        def _():
            close(i - 1)

        @pl.when(i > 0)
        def _():
            distant(i - 1)

        @pl.when(i == kv)
        def _():
            for r in range(near):
                p_buf[r] = part[r * seq:(r + 1) * seq].astype(BF16).reshape(2, half, 2 * rows)
                for h in range(SPLIT):
                    pcopy(r, h).start()

        @pl.when(i == jnp.where(outer, kv + 2, steps))
        def _():
            for r in range(near, group):
                finish(r, 0)

        return 0

    lax.fori_loop(0, steps + 1, step, 0)
    for r in range(near):
        for h in range(SPLIT):
            finish(r, h)
    for h in range(1, SPLIT):
        for r in range(near, group):
            finish(r, h)

    squares = jnp.zeros((1, 1), F32)
    for j in range(kv):
        dwcopy(j).wait_recv()
        a = acc[j, 0:rows] + wr[j].astype(F32)
        acc[j, 0:rows] = a
        squares = squares + jnp.sum(a * a, keepdims=True)
    sq[me] = jnp.broadcast_to(squares, (1, 128))

    def sqcopy(e, slot):
        return rcopy(sq.at[slot], sq.at[slot], sq_s.at[e], sq_r.at[slot], to(e // 2, e % 2))

    def sqsend(i, _):
        sqcopy((me + i) % total_devices, me).start()
        return 0

    lax.fori_loop(1, total_devices, sqsend, 0)

    for r in range(1, group):
        e = member(r)
        for f in range(2):
            xcopy(r, f).wait_send()
            for h in range(SPLIT):
                dxcopy(r, f, h, d).wait_send()
                dxcopy(r, f, h, e if f == 0 else other_half(e)).wait_recv()
    dx_store = pltpu.make_async_copy(dx_ref, dx_out, dxo_s)
    dx_store.start()
    for r in range(group):
        xfwd(r).wait_send()
        for h in range(SPLIT):
            pcopy(r, h).wait_send()

    def drain_g(j, _):
        wcopy(j).wait_send()
        dwcopy(j).wait_send()
        xncopy(j).wait_send()
        for i in range(2):
            ddcopy(i, j).wait_send()
        for h in range(SPLIT):
            colcopy(h, j).wait_send()
            relay(h, j).wait_send()
            for i in range(2):
                fardd(i, h, j).wait_send()
        return 0

    lax.fori_loop(0, kv, drain_g, 0)

    def drain(i, _):
        e = (me + i) % total_devices
        sqcopy(e, me).wait_send()
        sqcopy(e, e).wait_recv()
        return 0

    lax.fori_loop(1, total_devices, drain, 0)
    total = jnp.sum(sq[...], axis=0)[0:1, 0:1]
    factor = 1.0 / jnp.maximum(jnp.sqrt(total / total_entries), 1.0)
    for copy in momentum:
        copy.wait()
    stores = []
    for j in range(kv):
        cq = slice(j * gq, (j + 1) * gq)
        ck = slice(j * HEAD_SIZE, (j + 1) * HEAD_SIZE)
        for i, (buf, dst, cut, lo, hi) in enumerate((
            (mq, vq_out, cq, 0, gq),
            (mk, vk_out, ck, gq, gq + HEAD_SIZE),
            (mv, vv_out, ck, gq + HEAD_SIZE, wide),
        )):
            buf[:, cut] = 0.9 * buf[:, cut] + factor * acc[j, 0:rows, lo:hi]
            stores.append(pltpu.make_async_copy(buf.at[:, cut], dst.at[:, cut], vo_s.at[j, i]))
            stores[-1].start()
    for copy in (dx_store, *stores):
        copy.wait()


def fused(nd, nt, inputs, q, k, v, do, wq, wk, wv, mq, mk, mv):
    seq = q.shape[1]
    kv = k.shape[2] // HEAD_SIZE
    wide = (q.shape[2] + 2 * k.shape[2]) // kv
    rows = wq.shape[0]
    half = seq // nt
    group = nd // 2
    total_entries = float(rows * nd * kv * wide * nt)
    dma = pltpu.SemaphoreType.DMA
    return pl.pallas_call(
        functools.partial(kernel, nd, total_entries),
        out_shape=(
            jax.ShapeDtypeStruct(inputs.shape, BF16),
            jax.ShapeDtypeStruct(wq.shape, F32),
            jax.ShapeDtypeStruct(wk.shape, F32),
            jax.ShapeDtypeStruct(wv.shape, F32),
        ),
        in_specs=[pl.BlockSpec(memory_space=pltpu.HBM)] * 11,
        out_specs=(pl.BlockSpec(memory_space=pltpu.HBM),) * 4,
        scratch_shapes=[
            pltpu.VMEM((kv, group, nt, half, wide), BF16),
            pltpu.VMEM((group, nt, half, 2 * rows), BF16),
            pltpu.VMEM((kv, 2 * rows, wide), BF16),
            pltpu.VMEM((kv, 2 * rows, wide), F32),
            pltpu.VMEM((group // 2 * seq, 2 * rows), F32),
            pltpu.VMEM((SPLIT, group // 2 * seq // SPLIT, 2 * rows), F32),
            pltpu.VMEM((group, nt, half, 2 * rows), BF16),
            pltpu.VMEM((group, half, 2 * rows), BF16),
            pltpu.VMEM((group, half, 2 * rows), BF16),
            pltpu.VMEM((kv, rows, wide), BF16),
            pltpu.VMEM((kv, rows, wide), BF16),
            pltpu.VMEM((nd * nt, 1, 128), F32),
            pltpu.VMEM(mq.shape, F32),
            pltpu.VMEM(mk.shape, F32),
            pltpu.VMEM(mv.shape, F32),
            pltpu.VMEM(inputs.shape, BF16),
            pltpu.VMEM(q.shape, BF16),
            pltpu.VMEM(k.shape, BF16),
            pltpu.VMEM(v.shape, BF16),
            pltpu.VMEM(do.shape, BF16),
            pltpu.VMEM(inputs.shape, BF16),
            dma((group, 2)), dma((group, 2)), dma((group,)), dma((group,)),
            dma((kv,)), dma((kv,)), dma((SPLIT, kv)), dma((SPLIT, kv)),
            dma((SPLIT, kv)), dma((SPLIT, kv)), dma((2, SPLIT, kv)), dma((2, SPLIT, kv)),
            dma((kv,)), dma((kv,)), dma((2, kv)), dma((2, kv)),
            dma((group, SPLIT)), dma((group, SPLIT)), dma((group, 2, SPLIT)), dma((group, 2, SPLIT)),
            dma((kv,)), dma((kv,)), dma((nd * nt,)), dma((nd * nt,)), dma((3,)), dma((5,)), dma((kv, 3)), dma, dma((kv, 3)),
        ],
        compiler_params=pltpu.CompilerParams(
            collective_id=0, has_side_effects=True, vmem_limit_bytes=60 * 1024 * 1024
        ),
    )(inputs, q, k, v, do, wq, wk, wv, mq, mk, mv)


def pieces_of(shape):
    axis = len(shape) - 2
    step = shape[axis] // 2
    return [(slice(None),) * axis + (slice(i * step, (i + 1) * step),) for i in range(2)]


def hand_kernel(*refs):
    ins, outs, bufs, (get_s, put_s) = refs[0:4], refs[4:8], refs[8:12], refs[12:14]
    gets, puts = [], []
    for i in range(4):
        for k, cut in enumerate(pieces_of(ins[i].shape)):
            gets.append(pltpu.make_async_copy(ins[i].at[cut], bufs[i].at[cut], get_s.at[i, k]))
            puts.append(pltpu.make_async_copy(bufs[i].at[cut], outs[i].at[cut], put_s.at[i, k]))
    for get in gets:
        get.start()
    for get, put in zip(gets, puts):
        get.wait()
        put.start()
    for put in puts:
        put.wait()


def handed(*arrays):
    hbm = pl.BlockSpec(memory_space=pltpu.HBM)
    return pl.pallas_call(
        hand_kernel,
        out_shape=tuple(jax.ShapeDtypeStruct(a.shape, a.dtype) for a in arrays),
        in_specs=[hbm] * 4,
        out_specs=(hbm,) * 4,
        scratch_shapes=[pltpu.VMEM(a.shape, a.dtype) for a in arrays]
        + [pltpu.SemaphoreType.DMA((4, 2))] * 2,
        compiler_params=pltpu.CompilerParams(vmem_limit_bytes=60 * 1024 * 1024),
    )(*arrays)


def heads_backward(query_row_set, key_rows, value_rows, cotangent_rows):
    token_length = query_row_set.shape[0]
    kv_heads = key_rows.shape[1] // HEAD_SIZE
    group_width = query_row_set.shape[1] // HEAD_SIZE // kv_heads
    scaling = 1.0 / math.sqrt(HEAD_SIZE)
    query_quad = query_row_set.reshape(token_length, kv_heads, group_width, HEAD_SIZE)
    cotangent_quad = cotangent_rows.reshape(token_length, kv_heads, group_width, HEAD_SIZE)
    key_triple = key_rows.reshape(token_length, kv_heads, HEAD_SIZE)
    value_triple = value_rows.reshape(token_length, kv_heads, HEAD_SIZE)
    block_rows = min(token_length, 512)
    key_sums = jnp.zeros((token_length, kv_heads, HEAD_SIZE), F32)
    value_sums = jnp.zeros((token_length, kv_heads, HEAD_SIZE), F32)
    query_blocks = []
    for row_start in range(0, token_length, block_rows):
        row_end = row_start + block_rows
        query_block = query_quad[row_start:row_end]
        cotangent_block = cotangent_quad[row_start:row_end]
        key_block = key_triple[:row_end]
        value_block = value_triple[:row_end]
        scores = (
            jnp.einsum("ihgd,jhd->hgij", query_block, key_block, preferred_element_type=F32)
            * scaling
        )
        query_index = row_start + lax.broadcasted_iota(jnp.int32, (block_rows, row_end), 0)
        key_index = lax.broadcasted_iota(jnp.int32, (block_rows, row_end), 1)
        scores = jnp.where(query_index >= key_index, scores, -jnp.inf)
        maximum = jnp.max(scores, axis=-1, keepdims=True)
        exponent = jnp.exp(scores - maximum)
        softmax_rows = exponent / jnp.sum(exponent, axis=-1, keepdims=True)
        softmax_reduced = softmax_rows.astype(BF16)
        grad_softmax = jnp.einsum(
            "ihgd,jhd->hgij", cotangent_block, value_block, preferred_element_type=F32
        )
        row_delta = jnp.sum(softmax_rows * grad_softmax, axis=-1, keepdims=True)
        score_gradient = (softmax_rows * (grad_softmax - row_delta) * scaling).astype(BF16)
        query_blocks.append(
            jnp.einsum(
                "hgij,jhd->ihgd", score_gradient, key_block, preferred_element_type=F32
            ).astype(BF16)
        )
        key_sums = key_sums.at[:row_end].add(
            jnp.einsum(
                "xfwo,wxfp->oxp", score_gradient, query_block, preferred_element_type=F32
            )
        )
        value_sums = value_sums.at[:row_end].add(
            jnp.einsum(
                "xfwo,wxfp->oxp",
                softmax_reduced,
                cotangent_block,
                preferred_element_type=F32,
            )
        )
    grad_query = jnp.concatenate(query_blocks, axis=0).reshape(token_length, -1)
    key_gradient = key_sums.astype(BF16).reshape(token_length, -1)
    value_gradient = value_sums.astype(BF16).reshape(token_length, -1)
    return (grad_query, key_gradient, value_gradient)


def small(nd, nt, inputs, query_states, key_states, query_weight):
    seq = query_states.shape[1]
    cols = query_states.shape[2] + 2 * key_states.shape[2]
    held = nd * seq * cols * 2 + 10 * nd * seq * query_weight.shape[0]
    even = key_states.shape[2] % (2 * HEAD_SIZE) == 0
    return nt == 2 and nd == 16 and even and held < 36 * 1024 * 1024


def local(nd, nt, *args):
    inputs, q, k, v, do, wq, wk, wv, mq, mk, mv = args
    if small(nd, nt, inputs, q, k, wq):
        return handed(*fused(nd, nt, *args))
    else:
        query_cols = wq.shape[1]
        pair_cols = wk.shape[1]
        rows = wq.shape[0]
        weights = jnp.concatenate((wq, wk, wv), axis=1)
        grads = jnp.concatenate(heads_backward(q[0], k[0], v[0], do[0]), axis=1)
        all_grads = lax.all_gather(grads, "dp", axis=0, tiled=True)
        pieces = lax.all_to_all(inputs[0], "dp", 1, 0, tiled=True)
        pieces = pieces.reshape(nd, -1, rows)
        all_inputs = lax.all_gather(pieces, "tensor", axis=1, tiled=True).reshape(-1, rows)
        summed = dot(all_inputs, all_grads, 0, 0)
        parts = dot(all_grads, weights, 1, 1).astype(BF16).reshape(nd, -1, rows)
        mine = lax.psum_scatter(parts, "tensor", scatter_dimension=1, tiled=True)
        grad_inputs = lax.all_to_all(mine.reshape(-1, rows), "dp", 0, 1, tiled=True)[None]
        total = lax.psum(jnp.sum(summed * summed), ("dp", "tensor"))
        factor = 1.0 / jnp.maximum(jnp.sqrt(total / (summed.size * nd * nt)), 1.0)
        gq = summed[:, :query_cols]
        gk = summed[:, query_cols:query_cols + pair_cols]
        gv = summed[:, query_cols + pair_cols:]
    return (
        grad_inputs,
        0.9 * mq + factor * gq,
        0.9 * mk + factor * gk,
        0.9 * mv + factor * gv,
    )


def solution(mesh):
    nd, nt = mesh.shape["dp"], mesh.shape["tensor"]
    saved = P("dp", None, "tensor")
    tokens = P("dp", "tensor", None)
    weight = P("dp", "tensor")
    return jax.shard_map(
        functools.partial(local, nd, nt),
        mesh=mesh,
        in_specs=(tokens,) + (saved,) * 4 + (weight,) * 6,
        out_specs=(tokens,) + (weight,) * 3,
        check_vma=False,
    )
```
